32 devices in a mesh: data: 2 (over x), tp: 4 (over z), sp: 4 (over y, core).
Axes of the slice: x: 2, y: 2, z: 4, core: 2. Of those that a mesh axis runs over, the one named last changes fastest.
Arguments:
- x: bfloat16 [2, 16, 256, 5120], P('data', 'sp', 'tp'), parts along dimension 0
- ln_gain: float32 [2, 2, 5120], replicated
- ln_bias: float32 [2, 2, 5120], replicated
- w_qkv: bfloat16 [2, 5120, 3, 40, 128], P(None, None, None, 'tp')
- w_out: bfloat16 [2, 40, 128, 5120], P(None, 'tp')
- w_up: bfloat16 [2, 5120, 13824], P(None, None, 'tp')
- w_down: bfloat16 [2, 13824, 5120], P(None, 'tp')
Outputs:
- output: bfloat16 [2, 16, 256, 5120], P('data', 'sp', 'tp'), parts along dimension 0
There are 2 independent parts. The reference program is written for one: setup_inputs(seed, part) draws one part's arguments, and reference() takes and returns one part's arrays. A program takes and returns all parts, laid end to end along the dimension named above; an argument that names none is the same for every part.
All inputs are finite; a program needn't handle non-finite values.
Results may differ from the reference program's by a relative error of at most 0.0172211.
Values are sent between devices in bfloat16 or wider.
A program may use at most 1 GiB of HBM per device.

```python
import jax
import jax.numpy as jnp
from jax import lax

MODEL_WIDTH = 5120
HEAD_COUNT = 40
HIDDEN_WIDTH = 13824
BATCH_SIZE = 1
FRAME_COUNT = 16
PATCH_COUNT = 256
HEAD_SIZE = MODEL_WIDTH // HEAD_COUNT


def setup_inputs(seed: int = 0, part: int = 0) -> dict:
    part_key = jax.random.fold_in(jax.random.key(seed), part)
    act_keys = jax.random.split(part_key, 3)
    frame_part = jax.random.normal(act_keys[0], (BATCH_SIZE, FRAME_COUNT, 1, MODEL_WIDTH), jnp.float32)
    patch_part = jax.random.normal(act_keys[1], (BATCH_SIZE, 1, PATCH_COUNT, MODEL_WIDTH), jnp.float32)
    token_part = jax.random.normal(act_keys[2], (BATCH_SIZE, FRAME_COUNT, PATCH_COUNT, MODEL_WIDTH), jnp.float32)
    latent = 0.8 * frame_part + 0.6 * patch_part + 0.5 * token_part
    weight_keys = jax.random.split(jax.random.key(seed + 1), 6)
    ln_gain = 1.0 + 0.25 * jax.random.normal(weight_keys[0], (2, 2, MODEL_WIDTH), jnp.float32)
    ln_bias = 0.4 * jax.random.normal(weight_keys[1], (2, 2, MODEL_WIDTH), jnp.float32)
    qkv_scale = jnp.array([1.4, 1.4, 1.0], jnp.float32).reshape(1, 1, 3, 1, 1) * MODEL_WIDTH ** -0.5
    w_qkv = jax.random.normal(weight_keys[2], (2, MODEL_WIDTH, 3, HEAD_COUNT, HEAD_SIZE), jnp.float32) * qkv_scale
    w_out = jax.random.normal(weight_keys[3], (2, HEAD_COUNT, HEAD_SIZE, MODEL_WIDTH), jnp.float32) * MODEL_WIDTH ** -0.5
    w_up = jax.random.normal(weight_keys[4], (2, MODEL_WIDTH, HIDDEN_WIDTH), jnp.float32) * MODEL_WIDTH ** -0.5
    w_down = jax.random.normal(weight_keys[5], (2, HIDDEN_WIDTH, MODEL_WIDTH), jnp.float32) * HIDDEN_WIDTH ** -0.5
    return {"x": latent.astype(jnp.bfloat16), "ln_gain": ln_gain, "ln_bias": ln_bias, "w_qkv": w_qkv.astype(jnp.bfloat16), "w_out": w_out.astype(jnp.bfloat16), "w_up": w_up.astype(jnp.bfloat16), "w_down": w_down.astype(jnp.bfloat16)}


def layer_norm(residual, gain, shift):
    centered = residual.astype(jnp.float32)
    centered = centered - jnp.mean(centered, axis=-1, keepdims=True)
    variance = jnp.mean(centered * centered, axis=-1, keepdims=True)
    return (centered * lax.rsqrt(variance + 1e-6) * gain + shift).astype(jnp.bfloat16)


def row_group(n_rows, row_cost):
    best = 1
    for candidate in range(1, n_rows + 1):
        if n_rows % candidate == 0 and candidate * row_cost <= 2 ** 24:
            best = candidate
    return best


def attend(query, keys, values):
    n_rows, length = query.shape[0], query.shape[1]
    group = row_group(n_rows, HEAD_COUNT * length * length)

    def one_group(blocks):
        q_rows, k_rows, v_rows = blocks
        scores = jnp.einsum("rqhk,rshk->rhqs", q_rows.astype(jnp.float32), k_rows.astype(jnp.float32)) * HEAD_SIZE ** -0.5
        attn_prob = jax.nn.softmax(scores, axis=-1).astype(jnp.bfloat16)
        mixed = jnp.einsum("rhqs,rshk->rqhk", attn_prob.astype(jnp.float32), v_rows.astype(jnp.float32))
        return mixed.astype(jnp.bfloat16)

    grouped = tuple(tensor.reshape((n_rows // group, group) + tensor.shape[1:]) for tensor in (query, keys, values))
    mixed_all = lax.map(one_group, grouped)
    return mixed_all.reshape(query.shape)


def transformer_block(residual, gain, shift, w_qkv, w_out, w_up, w_down):
    batch_n, rows_n, length, width = residual.shape
    normed = layer_norm(residual, gain[0], shift[0]).reshape(-1, width)
    qkv_proj = jnp.dot(normed, w_qkv.reshape(width, 3 * width), preferred_element_type=jnp.float32).astype(jnp.bfloat16)
    qkv_proj = qkv_proj.reshape(batch_n * rows_n, length, 3, HEAD_COUNT, HEAD_SIZE)
    attended = attend(qkv_proj[:, :, 0], qkv_proj[:, :, 1], qkv_proj[:, :, 2])
    attn_proj = jnp.dot(attended.reshape(-1, width), w_out.reshape(width, width), preferred_element_type=jnp.float32).astype(jnp.bfloat16)
    hidden = (residual.astype(jnp.float32) + attn_proj.reshape(residual.shape).astype(jnp.float32)).astype(jnp.bfloat16)
    normed_mlp = layer_norm(hidden, gain[1], shift[1]).reshape(-1, width)
    up_proj = jnp.dot(normed_mlp, w_up, preferred_element_type=jnp.float32).astype(jnp.bfloat16)
    gelu_out = jax.nn.gelu(up_proj.astype(jnp.float32), approximate=True).astype(jnp.bfloat16)
    down_proj = jnp.dot(gelu_out, w_down, preferred_element_type=jnp.float32).astype(jnp.bfloat16)
    return (hidden.astype(jnp.float32) + down_proj.reshape(residual.shape).astype(jnp.float32)).astype(jnp.bfloat16)


def reference(x, ln_gain, ln_bias, w_qkv, w_out, w_up, w_down):
    spatial = transformer_block(x, ln_gain[0], ln_bias[0], w_qkv[0], w_out[0], w_up[0], w_down[0])
    temporal = transformer_block(spatial.transpose(0, 2, 1, 3), ln_gain[1], ln_bias[1], w_qkv[1], w_out[1], w_up[1], w_down[1])
    return temporal.transpose(0, 2, 1, 3)
```

```python
import functools

import jax
import jax.numpy as jnp
from jax import lax
from jax.experimental import pallas as pl
from jax.experimental.pallas import tpu as pltpu
from jax.sharding import PartitionSpec as P

bf16, f32 = jnp.bfloat16, jnp.float32
MESH = pl.DeviceIdType.MESH
LINE = 4
NB = 256
UB = 384
RB = 16
VMEM_LIMIT = 66_500_000


def shift(axis_bits):
    data, sp = lax.axis_index("data"), lax.axis_index("sp")
    fx, fy, fc = axis_bits
    data = 1 - data if fx else data
    y, core = sp // 2, sp % 2
    y = 1 - y if fy else y
    core = 1 - core if fc else core
    return {"data": data, "sp": y * 2 + core}


PEERS = ((0, 0, 1), (0, 1, 0), (1, 0, 0), (1, 1, 0))


class Line:
    def __init__(self):
        self.z = lax.axis_index("tp")

    def exists(self, direction):
        return self.z < LINE - 1 if direction == 0 else self.z > 0

    def source_exists(self, direction):
        return self.z > 0 if direction == 0 else self.z < LINE - 1

    def target(self, direction):
        return {"tp": self.z + 1 if direction == 0 else self.z - 1}

    def origin(self, direction, hop):
        return self.z - hop if direction == 0 else self.z + hop

    def sends(self, direction, hop):
        o = self.origin(direction, hop)
        return jnp.logical_and(self.exists(direction), jnp.logical_and(o >= 0, o < LINE))

    def receives(self, direction, hop):
        o = self.origin(direction, hop + 1)
        return jnp.logical_and(o >= 0, o < LINE)


def remote(src, dst, send, recv, device):
    return pltpu.make_async_remote_copy(src_ref=src, dst_ref=dst, send_sem=send, recv_sem=recv, device_id=device, device_id_type=MESH)


class Gather:
    def __init__(self, line, own, slot, send, recv):
        self.line, self.own, self.slot, self.send, self.recv = line, own, slot, send, recv

    def copy(self, d, c, hop):
        o = jnp.clip(self.line.origin(d, hop), 0, LINE - 1)
        src = self.own(c) if hop == 0 else self.slot(c, o)
        return remote(src, self.slot(c, o), self.send.at[d, c, hop], self.recv.at[d, c, hop], self.line.target(d))

    def arrival(self, d, c, hop):
        o = jnp.clip(self.line.origin(d, hop + 1), 0, LINE - 1)
        here = self.slot(c, o)
        return remote(here, here, self.send.at[d, c, hop], self.recv.at[d, c, hop], self.line.target(d))

    def start(self, c, hop):
        for d in range(2):
            @pl.when(self.line.sends(d, hop))
            def _():
                self.copy(d, c, hop).start()

    def arrive(self, c, hop):
        for d in range(2):
            @pl.when(self.line.receives(d, hop))
            def _():
                self.arrival(d, c, hop).wait_recv()

    def relay(self, c, hop):
        self.arrive(c, hop - 1)
        self.start(c, hop)

    def finish(self, chunks):
        for c in range(chunks):
            for hop in range(LINE - 1):
                for d in range(2):
                    @pl.when(self.line.sends(d, hop))
                    def _():
                        self.copy(d, c, hop).wait_send()


def meet(line, peers):
    barrier = pltpu.get_barrier_semaphore()
    for d in range(2):
        @pl.when(line.exists(d))
        def _():
            pl.semaphore_signal(barrier, inc=1, device_id=line.target(d), device_id_type=MESH)
    for p in peers:
        pl.semaphore_signal(barrier, inc=1, device_id=shift(p), device_id_type=MESH)
    pl.semaphore_wait(barrier, jnp.where(jnp.logical_or(line.z == 0, line.z == LINE - 1), 1, 2) + len(peers))


def normalize(src, dst, gain, bias):
    def rows(i, _):
        at = pl.ds(pl.multiple_of(i * RB, RB), RB)
        u = src[at, :].astype(f32)
        u = u - jnp.mean(u, axis=-1, keepdims=True)
        var = jnp.mean(u * u, axis=-1, keepdims=True)
        dst[at, :] = (u * lax.rsqrt(var + 1e-6) * gain[...] + bias[...]).astype(bf16)
        return 0

    lax.fori_loop(0, src.shape[0] // RB, rows, 0)


def tiles(count, copies, compute):
    for when, copy in copies(0, 0):
        when(copy.start) if when else copy.start()

    def step(n, _):
        slot = lax.rem(n, 2)

        @pl.when(n + 1 < count)
        def _():
            for when, copy in copies(n + 1, 1 - slot):
                when(copy.start) if when else copy.start()

        for when, copy in copies(n, slot):
            when(copy.wait) if when else copy.wait()
        compute(n, slot)
        return 0

    lax.fori_loop(0, count, step, 0)


def gather_attend(cfg, b, x, gain, bias, wq, wo, r_out, o_out, wg, rv, nv, wbuf, qkv, ov, xs, xr, ws, wr, ps, pr, fs, fr, ls, ts):
    chunks, rows, width = x.shape
    tokens = rows * LINE
    hk = wo.shape[1]
    heads = hk // 128
    cols = width // 8
    line = Line()
    z = line.z
    place = lax.axis_index("data") * 4 + lax.axis_index("sp")
    at_cols = lambda p: pl.ds(pl.multiple_of(p * cols, 128), cols)
    g = Gather(line, lambda c: x.at[c], lambda c, o: r_out.at[c, o], xs, xr)
    w = Gather(line, lambda c: wo.at[b, :, at_cols(place)], lambda c, o: wg.at[o, :, at_cols(place)], ws, wr)

    def peer_place(k):
        dev = shift(PEERS[k])
        return dev["data"] * 4 + dev["sp"]

    def plane(d, hop, k, p):
        o = jnp.clip(line.origin(d, hop + 1), 0, LINE - 1)
        return wg.at[o, :, at_cols(p)]

    def spread(hop):
        for d in range(2):
            @pl.when(line.receives(d, hop))
            def _():
                for k in range(4):
                    ref = plane(d, hop, k, place)
                    remote(ref, ref, ps.at[d, hop, k], pr.at[d, hop, k], shift(PEERS[k])).start()

    def forward(hop):
        for d in range(2):
            @pl.when(line.receives(d, hop))
            def _():
                for k in range(1, 4):
                    ref = plane(d, hop, k, peer_place(k))
                    remote(ref, ref, ps.at[d, hop, k], pr.at[d, hop, k], shift(PEERS[k])).wait_recv()
                    remote(ref, ref, fs.at[d, hop, k - 1], fr.at[d, hop, k - 1], shift(PEERS[0])).start()

    def plane_finish():
        for hop in range(LINE - 1):
            for d in range(2):
                @pl.when(line.receives(d, hop))
                def _():
                    for k in range(4):
                        ref = plane(d, hop, k, place)
                        remote(ref, ref, ps.at[d, hop, k], pr.at[d, hop, k], shift(PEERS[k])).wait_send()
                    ref = plane(d, hop, 0, peer_place(0))
                    remote(ref, ref, ps.at[d, hop, 0], pr.at[d, hop, 0], shift(PEERS[0])).wait_recv()
                    for k in range(1, 4):
                        ref = plane(d, hop, k, peer_place(k))
                        remote(ref, ref, fs.at[d, hop, k - 1], fr.at[d, hop, k - 1], shift(PEERS[0])).wait_send()
                        far = shift(tuple(m ^ n for m, n in zip(PEERS[k], PEERS[0])))
                        ref = plane(d, hop, k, far["data"] * 4 + far["sp"])
                        remote(ref, ref, fs.at[d, hop, k - 1], fr.at[d, hop, k - 1], shift(PEERS[0])).wait_recv()

    def load(c):
        copies = []
        for s in range(LINE):
            there = rv.at[pl.ds(s * rows, rows), :]
            copies.append((z == s, pltpu.make_async_copy(x.at[c], there, ls.at[s]), pltpu.make_async_copy(r_out.at[c, s], there, ls.at[s])))
        for mine, a, o in copies:
            pl.when(mine)(a.start)
            pl.when(jnp.logical_not(mine))(o.start)
        for _, a, _ in copies:
            a.wait()

    def own_rows(c):
        at = pl.ds(pl.multiple_of(z * rows, rows), rows)
        return pltpu.make_async_copy(rv.at[at, :], r_out.at[c, z], ls.at[LINE])

    def work(c):
        g.arrive(c, 2)
        load(c)
        own_rows(c).start()
        normalize(rv, nv, gain, bias)
        pairs = heads // 2

        def copies(n, slot):
            part, pair = n // pairs, n % pairs
            return [(None, pltpu.make_async_copy(wq.at[b, part, pair * 2 + i], wbuf.at[slot, :, pl.ds(i * 128, 128)], ts.at[slot, i])) for i in range(2)]

        def compute(n, slot):
            at = pl.ds(pl.multiple_of(n * NB, NB), NB)
            qkv[:, at] = jnp.dot(nv[...], wbuf[slot], preferred_element_type=f32).astype(bf16)

        tiles(3 * pairs, copies, compute)
        if cfg["step"]:
            step = cfg["step"]
            key = lambda t: t // rows * step + t % step
            mask = key(lax.broadcasted_iota(jnp.int32, (tokens, tokens), 0)) == key(lax.broadcasted_iota(jnp.int32, (tokens, tokens), 1))

        def head(h, _):
            at = lambda part: pl.ds(pl.multiple_of((part * heads + h) * 128, 128), 128)
            s = lax.dot_general(qkv[:, at(0)], qkv[:, at(1)], (((1,), (1,)), ((), ())), preferred_element_type=f32) * 128**-0.5
            if cfg["step"]:
                s = jnp.where(mask, s, -1e30)
            e = jnp.exp(s - jnp.max(s, axis=-1, keepdims=True))
            p = (e * (1.0 / jnp.sum(e, axis=-1, keepdims=True))).astype(bf16)
            ov[:, pl.ds(pl.multiple_of(h * 128, 128), 128)] = jnp.dot(p, qkv[:, at(2)], preferred_element_type=f32).astype(bf16)
            return 0

        lax.fori_loop(0, heads, head, 0)
        out = pltpu.make_async_copy(ov, o_out.at[c], ls.at[LINE + 1])
        out.start()
        own_rows(c).wait()
        out.wait()

    meet(line, PEERS)
    w.start(0, 0)
    g.start(0, 0)
    w.relay(0, 1)
    spread(0)
    g.start(1, 0)
    g.relay(0, 1)
    g.start(2, 0)
    w.relay(0, 2)
    spread(1)
    g.relay(0, 2)
    g.relay(1, 1)
    g.start(3, 0)
    w.arrive(0, 2)
    spread(2)
    g.relay(1, 2)
    g.relay(2, 1)
    work(0)
    g.relay(2, 2)
    g.relay(3, 1)
    work(1)
    g.relay(3, 2)
    forward(0)
    work(2)
    forward(1)
    work(3)
    forward(2)
    g.finish(chunks)
    w.finish(1)
    plane_finish()


def mix_feed(b, o, r, wo, wg, gain, bias, wu, wd, y, og, part, rv, nv, gv, mine, wbuf, got, add, pst, os_, or_, rs, rr, ls, ts, ds):
    chunks, tokens, hk = o.shape
    rows = tokens // LINE
    width, hidden = wu.shape[1:]
    line = Line()
    z = line.z
    g = Gather(line, lambda c: o.at[c], lambda c, s: og.at[c, s], os_, or_)

    def out_copies(n, slot):
        cols = pl.ds(pl.multiple_of(n * NB, NB), NB)
        copies = []
        for s in range(LINE):
            there = wbuf.at[slot, pl.ds(s * hk, hk), pl.ds(0, NB)]
            copies.append((pl.when(z == s), pltpu.make_async_copy(wo.at[b, :, cols], there, ts.at[slot, s])))
            copies.append((pl.when(z != s), pltpu.make_async_copy(wg.at[s, :, cols], there, ts.at[slot, s])))
        return copies

    def load(c):
        copies = [pltpu.make_async_copy(r.at[c], rv, ls.at[LINE])]
        for c_ in copies:
            c_.start()
        both = []
        for s in range(LINE):
            there = nv.at[:, pl.ds(s * hk, hk)]
            both.append((z == s, pltpu.make_async_copy(o.at[c], there, ls.at[s]), pltpu.make_async_copy(og.at[c, s], there, ls.at[s])))
        for own, a, other in both:
            pl.when(own)(a.start)
            pl.when(jnp.logical_not(own))(other.start)
        for _, a, _ in both:
            a.wait()
        copies[0].wait()

    def project(c):
        load(c)

        def compute(n, slot):
            at = pl.ds(pl.multiple_of(n * NB, NB), NB)
            a = jnp.dot(nv[...], wbuf[slot, :, :NB], preferred_element_type=f32).astype(bf16)
            rv[:, at] = (rv[:, at].astype(f32) + a.astype(f32)).astype(bf16)

        tiles(width // NB, out_copies, compute)
        normalize(rv, nv, gain, bias)
        mine[c] = rv[pl.ds(pl.multiple_of(z * rows, rows), rows), :]

    def up(c):
        def copies(n, slot):
            cols = pl.ds(pl.multiple_of(n * UB, 128), UB)
            return [(None, pltpu.make_async_copy(wu.at[b, :, cols], wbuf.at[slot], ts.at[slot, 0]))]

        def compute(n, slot):
            u = jnp.dot(nv[...], wbuf[slot], preferred_element_type=f32).astype(bf16).astype(f32)
            gv[:, pl.ds(pl.multiple_of(n * UB, 128), UB)] = jax.nn.gelu(u, approximate=True).astype(bf16)

        tiles(hidden // UB, copies, compute)

    def store(c, n, slot):
        cols = pl.ds(pl.multiple_of(n * NB, NB), NB)
        return pltpu.make_async_copy(pst.at[slot], part.at[c, :, cols], ds.at[slot])

    def down(c):
        count = width // NB

        def copies(n, slot):
            cols = pl.ds(pl.multiple_of(n * NB, NB), NB)
            return [(None, pltpu.make_async_copy(wd.at[b, :, cols], wbuf.at[slot, pl.ds(0, hidden), pl.ds(0, NB)], ts.at[slot, 0]))]

        def compute(n, slot):
            @pl.when(n >= 2)
            def _():
                store(c, n - 2, slot).wait()

            pst[slot] = jnp.dot(gv[...], wbuf[slot, :hidden, :NB], preferred_element_type=f32)
            store(c, n, slot).start()

        tiles(count, copies, compute)
        for n in (count - 2, count - 1):
            store(c, n, n % 2).wait()

    def term(c, t):
        return part.at[c, pl.ds(pl.multiple_of(t * rows, rows), rows), :]

    def hop_copy(d, c, far, src):
        return remote(src, got.at[d, c, LINE - 1 - far], rs.at[d, c, LINE - 1 - far], rr.at[d, c, LINE - 1 - far], line.target(d))

    def first(d):
        return z == 0 if d == 0 else z == LINE - 1

    def far_target(d, far):
        return z + far if d == 0 else z - far

    def reduce_start(c):
        for far in range(LINE - 1, 0, -1):
            for d in range(2):
                @pl.when(first(d))
                def _():
                    hop_copy(d, c, far, term(c, far if d == 0 else LINE - 1 - far)).start()

    def middle(d, far):
        t = far_target(d, far - 1)
        return jnp.logical_and(jnp.logical_not(first(d)), jnp.logical_and(t >= 0, t < LINE))

    def reduce_relay(c, far):
        for d in range(2):
            @pl.when(middle(d, far))
            def _():
                t = jnp.clip(far_target(d, far - 1), 0, LINE - 1)
                fetch = pltpu.make_async_copy(term(c, t), add, ls.at[LINE + 1])
                fetch.start()
                slot = got.at[d, c, LINE - 1 - far]
                hop_copy(d, c, far, slot).wait_recv()
                fetch.wait()

                def some(i, _):
                    at = pl.ds(pl.multiple_of(i * RB, RB), RB)
                    slot[at, :] = slot[at, :] + add[at, :]
                    return 0

                lax.fori_loop(0, rows // RB, some, 0)
                hop_copy(d, c, far - 1, slot).start()

    def result(c):
        return pltpu.make_async_copy(mine.at[c], y.at[c], ls.at[LINE + 2])

    def reduce_finish(c):
        fetch = pltpu.make_async_copy(term(c, z), add, ls.at[LINE + 1])
        fetch.start()
        for d in range(2):
            @pl.when(jnp.logical_not(first(d)))
            def _():
                hop_copy(d, c, 1, got.at[d, c, LINE - 2]).wait_recv()
        fetch.wait()

        def some(i, _):
            at = pl.ds(pl.multiple_of(i * RB, RB), RB)
            for d in range(2):
                @pl.when(jnp.logical_not(first(d)))
                def _():
                    add[at, :] = add[at, :] + got[d, c, LINE - 2, at, :]
            m = add[at, :].astype(bf16)
            mine[c, at, :] = (mine[c, at, :].astype(f32) + m.astype(f32)).astype(bf16)
            return 0

        lax.fori_loop(0, rows // RB, some, 0)
        result(c).start()
        result(c).wait()

    def reduce_sent(c):
        for far in range(LINE - 1, 0, -1):
            for d in range(2):
                @pl.when(first(d))
                def _():
                    hop_copy(d, c, far, term(c, 0)).wait_send()
                if far > 1:
                    @pl.when(middle(d, far))
                    def _():
                        hop_copy(d, c, far - 1, got.at[d, c, LINE - 1 - far]).wait_send()

    meet(line, ())
    g.start(0, 0)
    g.relay(0, 1)
    g.start(1, 0)
    g.relay(0, 2)
    g.relay(1, 1)
    g.start(2, 0)
    g.arrive(0, 2)
    project(0)
    g.relay(1, 2)
    g.relay(2, 1)
    g.start(3, 0)
    up(0)
    g.relay(2, 2)
    g.relay(3, 1)
    down(0)
    reduce_start(0)
    g.relay(3, 2)
    g.arrive(1, 2)
    project(1)
    up(1)
    reduce_relay(0, 3)
    down(1)
    reduce_start(1)
    reduce_relay(0, 2)
    g.arrive(2, 2)
    project(2)
    reduce_finish(0)
    up(2)
    down(2)
    reduce_start(2)
    reduce_relay(1, 3)
    reduce_relay(1, 2)
    g.arrive(3, 2)
    project(3)
    up(3)
    reduce_finish(1)
    down(3)
    reduce_start(3)
    reduce_relay(2, 3)
    reduce_relay(2, 2)
    reduce_finish(2)
    reduce_relay(3, 3)
    reduce_relay(3, 2)
    reduce_finish(3)
    g.finish(chunks)
    for c in range(chunks):
        reduce_sent(c)


ANY = pl.BlockSpec(memory_space=pl.ANY)
VMEM = pl.BlockSpec(memory_space=pltpu.VMEM)
DMA = pltpu.SemaphoreType.DMA


def call_gather_attend(b, step, x, gain, bias, wq, wo):
    chunks, rows, width = x.shape
    hk, tokens = wo.shape[1], rows * LINE
    hops = LINE - 1
    return pl.pallas_call(
        functools.partial(gather_attend, {"step": step}, b),
        out_shape=(
            jax.ShapeDtypeStruct((chunks, LINE, rows, width), bf16),
            jax.ShapeDtypeStruct((chunks, tokens, hk), bf16),
            jax.ShapeDtypeStruct((LINE, hk, width), bf16),
        ),
        in_specs=[ANY, VMEM, VMEM, ANY, ANY],
        out_specs=(ANY, ANY, ANY),
        scratch_shapes=[
            pltpu.VMEM((tokens, width), bf16), pltpu.VMEM((tokens, width), bf16), pltpu.VMEM((2, width, NB), bf16),
            pltpu.VMEM((tokens, 3 * hk), bf16), pltpu.VMEM((tokens, hk), bf16),
            DMA((2, chunks, hops)), DMA((2, chunks, hops)), DMA((2, 1, hops)), DMA((2, 1, hops)),
            DMA((2, hops, 4)), DMA((2, hops, 4)), DMA((2, hops, 3)), DMA((2, hops, 3)), DMA((LINE + 2,)), DMA((2, 2)),
        ],
        compiler_params=pltpu.CompilerParams(collective_id=b, has_side_effects=True, vmem_limit_bytes=VMEM_LIMIT),
        name=f"gather_attend_{b}",
    )(x, gain, bias, wq, wo)


def call_mix_feed(b, o, r, wo, wg, gain, bias, wu, wd):
    chunks, tokens, hk = o.shape
    rows = tokens // LINE
    width, hidden = wu.shape[1:]
    hops = LINE - 1
    return pl.pallas_call(
        functools.partial(mix_feed, b),
        out_shape=(
            jax.ShapeDtypeStruct((chunks, rows, width), bf16),
            jax.ShapeDtypeStruct((chunks, LINE, tokens, hk), bf16),
            jax.ShapeDtypeStruct((chunks, tokens, width), f32),
        ),
        in_specs=[ANY, ANY, ANY, ANY, VMEM, VMEM, ANY, ANY],
        out_specs=(ANY, ANY, ANY),
        scratch_shapes=[
            pltpu.VMEM((tokens, width), bf16), pltpu.VMEM((tokens, width), bf16), pltpu.VMEM((tokens, hidden), bf16),
            pltpu.VMEM((chunks, rows, width), bf16), pltpu.VMEM((2, width, UB), bf16), pltpu.VMEM((2, chunks, hops, rows, width), f32),
            pltpu.VMEM((rows, width), f32), pltpu.VMEM((2, tokens, NB), f32),
            DMA((2, chunks, hops)), DMA((2, chunks, hops)), DMA((2, chunks, hops)), DMA((2, chunks, hops)),
            DMA((LINE + 3,)), DMA((2, LINE)), DMA((2,)),
        ],
        compiler_params=pltpu.CompilerParams(collective_id=2 + b, has_side_effects=True, vmem_limit_bytes=VMEM_LIMIT),
        name=f"mix_feed_{b}",
    )(o, r, wo, wg, gain, bias, wu, wd)[0]


def solution(mesh):
    act_spec = P("data", "sp", "tp", None)
    weight_specs = (P(), P(), P(None, None, None, "tp", None), P(None, "tp", None, None), P(None, None, "tp"), P(None, "tp", None))

    def device_program(x, ln_gain, ln_bias, w_qkv, w_out, w_up, w_down):
        _, frames, rows, width = x.shape
        wq = w_qkv.transpose(0, 2, 3, 1, 4)
        wo = w_out.reshape(2, -1, width)

        def block(b, r, step):
            row = lambda a, i: a[b, i][None]
            r_full, o, wg = call_gather_attend(b, step, r, row(ln_gain, 0), row(ln_bias, 0), wq, wo)
            r_full = r_full.reshape(r_full.shape[0], -1, width)
            return call_mix_feed(b, o, r_full, wo, wg, row(ln_gain, 1), row(ln_bias, 1), w_up, w_down)

        spatial = block(0, x[0], 0)
        per = rows // 4
        step = per // 4
        turned = lax.all_to_all(spatial, "sp", 1, 0, tiled=True)
        turned = turned.reshape(4 * frames, 4, step, width).transpose(1, 0, 2, 3).reshape(4, -1, width)
        temporal = block(1, turned, step)
        back = temporal.reshape(4, 4 * frames, step, width).transpose(1, 0, 2, 3).reshape(4 * frames, per, width)
        return lax.all_to_all(back, "sp", 0, 1, tiled=True)[None]

    return jax.shard_map(device_program, mesh=mesh, in_specs=(act_spec,) + weight_specs, out_specs=act_spec, check_vma=False)
```

```python
import functools

import jax
import jax.numpy as jnp
from jax import lax
from jax.experimental import pallas as pl
from jax.experimental.pallas import tpu as pltpu
from jax.sharding import PartitionSpec as P

bf16, f32 = jnp.bfloat16, jnp.float32
MESH = pl.DeviceIdType.MESH
LINE = 4
NB = 512
SLOTS = 3
RB = 16
LN_ROWS = 64
VMEM_LIMIT = 66_500_000


CORE, Y, X, Y_CORE = (0, 0, 1), (0, 1, 0), (1, 0, 0), (0, 1, 1)


def shift(flips):
    data, sp = lax.axis_index("data"), lax.axis_index("sp")
    y, core = sp // 2, sp % 2
    return {"data": 1 - data if flips[0] else data, "sp": (1 - y if flips[1] else y) * 2 + (1 - core if flips[2] else core)}


def place_of(device):
    return device["data"] * 4 + device["sp"]


class Line:
    def __init__(self):
        self.z = lax.axis_index("tp")

    def exists(self, direction):
        return self.z < LINE - 1 if direction == 0 else self.z > 0

    def source_exists(self, direction):
        return self.z > 0 if direction == 0 else self.z < LINE - 1

    def target(self, direction):
        return {"tp": self.z + 1 if direction == 0 else self.z - 1}

    def origin(self, direction, hop):
        return self.z - hop if direction == 0 else self.z + hop

    def sends(self, direction, hop):
        o = self.origin(direction, hop)
        return jnp.logical_and(self.exists(direction), jnp.logical_and(o >= 0, o < LINE))

    def receives(self, direction, hop):
        o = self.origin(direction, hop + 1)
        return jnp.logical_and(o >= 0, o < LINE)


def remote(src, dst, send, recv, device):
    return pltpu.make_async_remote_copy(src_ref=src, dst_ref=dst, send_sem=send, recv_sem=recv, device_id=device, device_id_type=MESH)


class Gather:
    def __init__(self, line, own, slot, send, recv):
        self.line, self.own, self.slot, self.send, self.recv = line, own, slot, send, recv

    def copy(self, d, c, hop):
        o = jnp.clip(self.line.origin(d, hop), 0, LINE - 1)
        src = self.own(c) if hop == 0 else self.slot(c, o)
        return remote(src, self.slot(c, o), self.send.at[d, c, hop], self.recv.at[d, c, hop], self.line.target(d))

    def arrival(self, d, c, hop):
        o = jnp.clip(self.line.origin(d, hop + 1), 0, LINE - 1)
        here = self.slot(c, o)
        return remote(here, here, self.send.at[d, c, hop], self.recv.at[d, c, hop], self.line.target(d))

    def start(self, c, hop, only=lambda d: True):
        for d in range(2):
            @pl.when(jnp.logical_and(self.line.sends(d, hop), only(d)))
            def _():
                self.copy(d, c, hop).start()

    def arrive(self, c):
        for hop in range(LINE - 1):
            for d in range(2):
                self.settle(d, c, hop)

    def settle(self, d, c, hop):
        passed_on = self.line.sends(d, hop + 1) if hop + 1 < LINE - 1 else False

        @pl.when(jnp.logical_and(self.line.receives(d, hop), jnp.logical_not(passed_on)))
        def _():
            self.arrival(d, c, hop).wait_recv()

    def relay(self, c, hop, only=lambda d: True, wait=True):
        for d in range(2):
            @pl.when(jnp.logical_and(self.line.sends(d, hop), only(d)))
            def _():
                if wait:
                    self.arrival(d, c, hop - 1).wait_recv()
                self.copy(d, c, hop).start()

    def finish(self, chunks):
        for c in range(chunks):
            for hop in range(LINE - 1):
                for d in range(2):
                    @pl.when(self.line.sends(d, hop))
                    def _():
                        self.copy(d, c, hop).wait_send()


def meet(line, peers):
    barrier = pltpu.get_barrier_semaphore()
    for d in range(2):
        @pl.when(line.exists(d))
        def _():
            pl.semaphore_signal(barrier, inc=1, device_id=line.target(d), device_id_type=MESH)
    for p in peers:
        pl.semaphore_signal(barrier, inc=1, device_id=shift(p), device_id_type=MESH)
    pl.semaphore_wait(barrier, jnp.where(jnp.logical_or(line.z == 0, line.z == LINE - 1), 1, 2) + len(peers))


def normalize(src, dst, gain, bias, start, count):
    block = min(count, LN_ROWS)

    def some(i, _):
        at = pl.ds(pl.multiple_of(start + i * block, RB), block)
        u = src[at, :].astype(f32)
        u = u - jnp.mean(u, axis=-1, keepdims=True)
        var = jnp.mean(u * u, axis=-1, keepdims=True)
        dst[at, :] = (u * lax.rsqrt(var + 1e-6) * gain[...] + bias[...]).astype(bf16)
        return 0

    lax.fori_loop(0, count // block, some, 0)


class Phase:
    def __init__(self, count, copies, compute, after=None, middle=None):
        self.count, self.copies, self.compute, self.after, self.middle = count, copies, compute, after, middle

    def start(self, n, slot):
        for when, copy in self.copies(n, slot):
            when(copy.start) if when else copy.start()

    def wait(self, n, slot):
        for when, copy in self.copies(n, slot):
            when(copy.wait) if when else copy.wait()


def run_phases(phases, prepare):
    flat = [(p, n) for p in phases for n in range(p.count)]
    ahead = SLOTS - 1
    for i in range(ahead):
        flat[i][0].start(flat[i][1], i)
    prepare()
    base = 0
    for p in phases:
        later = flat[base + p.count : base + p.count + ahead]

        def step(n, _):
            slot = lax.rem(base + n, SLOTS)
            if p.count > ahead:
                @pl.when(n + ahead < p.count)
                def _():
                    p.start(n + ahead, lax.rem(base + n + ahead, SLOTS))
            for j, (q, m) in enumerate(later):
                when = p.count + j - ahead
                if when >= 0:
                    @pl.when(n == when)
                    def _():
                        q.start(m, (base + p.count + j) % SLOTS)
            p.wait(n, slot)
            p.compute(n, slot)
            if p.middle:
                pl.when(n == min(p.count // 2 + 1, p.count - 1))(p.middle)
            return 0

        if p.count == 1:
            step(0, 0)
        else:
            lax.fori_loop(0, p.count, step, 0)
        if p.after:
            p.after()
        base += p.count


class PlaneGather:
    def __init__(self, line, own, wg, ws, wr, ps, pr, fs, fr):
        width = wg.shape[2]
        cols = width // 8
        self.line, self.wg, self.ps, self.pr, self.fs, self.fr = line, wg, ps, pr, fs, fr
        self.cols = lambda p: pl.ds(pl.multiple_of(p * cols, 128), cols)
        me = shift((0, 0, 0))
        self.place = place_of(me)
        self.core = lax.axis_index("sp") % 2
        self.along = Gather(line, lambda c: own.at[:, self.cols(self.place)], lambda c, o: wg.at[o, :, self.cols(self.place)], ws, wr)
        across, beside = shift(X), shift(Y)
        first_is_x = self.core == 0
        self.diagonal_device = {k: jnp.where(first_is_x, beside[k], across[k]) for k in across}
        self.diagonal_given = jnp.where(first_is_x, place_of(across), place_of(beside))
        self.sources = (place_of(shift(CORE)), place_of(beside), place_of(across), place_of(shift((1, 1, 0))))

    def each(self, hop, action, only=lambda d: True):
        for d in range(2):
            @pl.when(jnp.logical_and(self.line.receives(d, hop), only(d)))
            def _():
                o = jnp.clip(self.line.origin(d, hop + 1), 0, LINE - 1)
                action(d, lambda p: self.wg.at[o, :, self.cols(p)])

    def direct(self, d, hop, k, ref):
        return remote(ref, ref, self.ps.at[d, hop, k], self.pr.at[d, hop, k], shift((CORE, Y, X)[k]))

    def diagonal(self, d, hop, ref):
        return remote(ref, ref, self.ps.at[d, hop, 3], self.pr.at[d, hop, 3], self.diagonal_device)

    def pass_on(self, d, hop, k, ref):
        return remote(ref, ref, self.fs.at[d, hop, k - 1], self.fr.at[d, hop, k - 1], shift(CORE))

    def spread(self, hop, only=lambda d: True, wait="unless relayed"):
        def action(d, slab):
            if wait == "always":
                self.along.arrival(d, 0, hop).wait_recv()
            elif wait == "unless relayed":
                self.along.settle(d, 0, hop)
            for k in range(3):
                self.direct(d, hop, k, slab(self.place)).start()

        self.each(hop, action, only)

    def forward(self, hop, only=lambda d: True):
        def action(d, slab):
            for k in (1, 2):
                self.direct(d, hop, k, slab(self.sources[k])).wait_recv()
                self.pass_on(d, hop, k, slab(self.sources[k])).start()
            self.diagonal(d, hop, slab(self.diagonal_given)).start()

        self.each(hop, action, only)

    def forward_diagonal(self, hop, only=lambda d: True):
        def action(d, slab):
            self.diagonal(d, hop, slab(self.sources[3])).wait_recv()
            self.pass_on(d, hop, 3, slab(self.sources[3])).start()

        self.each(hop, action, only)

    def arrive(self, hops):
        for hop in hops:
            def action(d, slab):
                self.direct(d, hop, 0, slab(self.sources[0])).wait_recv()
                for k in (1, 2, 3):
                    p = self.sources[k]
                    self.pass_on(d, hop, k, slab(p + 1 - 2 * (p % 2))).wait_recv()

            self.each(hop, action)

    def finish(self, hops):
        for hop in hops:
            def action(d, slab):
                for k in range(3):
                    self.direct(d, hop, k, slab(self.place)).wait_send()
                self.diagonal(d, hop, slab(self.diagonal_given)).wait_send()
                for k in (1, 2, 3):
                    self.pass_on(d, hop, k, slab(self.sources[k])).wait_send()

            self.each(hop, action)


def block_kernel(b, step, *refs):
    names = ["x", "gains", "biases", "wq", "wo", "wu", "wd"] + ([] if b == 0 else ["wg_in"])
    names += ["turned", "r", "og", "o", "part"] + (["wg0", "wg1"] if b == 0 else ["wg1"])
    names += ["rv", "nv", "qkv", "ov", "gv", "mine", "wbuf", "far_got", "got", "add", "pst"]
    names += ["xs", "xr", "os", "or_", "rs", "rr", "vs", "vr", "ls", "ts", "ds", "hs", "hr", "ws", "wr", "ps", "pr", "fs", "fr"]
    v = dict(zip(names, refs, strict=True))
    x, r, o, og, part, turned = (v[k] for k in ("x", "r", "o", "og", "part", "turned"))
    wq, wo, wu, wd = (v[k] for k in ("wq", "wo", "wu", "wd"))
    rv, nv, qkv, ov, gv, mine, wbuf, far_got, got, add, pst = (v[k] for k in ("rv", "nv", "qkv", "ov", "gv", "mine", "wbuf", "far_got", "got", "add", "pst"))
    rs, rr, vs, vr, ls, ts, ds = (v[k] for k in ("rs", "rr", "vs", "vr", "ls", "ts", "ds"))
    wg = v[f"wg{b}"]
    chunks, rows, width = x.shape
    tokens = rows * LINE
    hk, hidden = wo.shape[1], wu.shape[2]
    heads = hk // 128
    line = Line()
    z = line.z
    xg = Gather(line, lambda c: x.at[c], lambda c, s: r.at[c, s], v["xs"], v["xr"])
    og_ = Gather(line, lambda c: o.at[c], lambda c, s: og.at[c, s], v["os"], v["or_"])
    w0, w1 = (PlaneGather(line, wo.at[i], v[f"wg{i}"], *(v[k].at[i] for k in ("ws", "wr", "ps", "pr", "fs", "fr"))) if i >= b else None for i in range(2))

    def rows_of(o):
        return pl.ds(pl.multiple_of(o * rows, rows), rows)

    def columns(n):
        return pl.ds(pl.multiple_of(n * NB, 128), NB)

    def load_r(c):
        copies = []
        for s in range(LINE):
            there = rv.at[pl.ds(s * rows, rows), :]
            copies.append((z == s, pltpu.make_async_copy(x.at[c], there, ls.at[s]), pltpu.make_async_copy(r.at[c, s], there, ls.at[s])))
        for own, a, other in copies:
            pl.when(own)(a.start)
            pl.when(jnp.logical_not(own))(other.start)
        for _, a, _ in copies:
            a.wait()

    per_tile = NB // 128

    def qkv_phase(c, first, count, wide, middle=None):
        def copies(n, slot):
            return [(None, pltpu.make_async_copy(wq.at[b, (first + n) * per_tile + i], wbuf.at[slot, :, pl.ds(i * 128, 128)], ts.at[slot, i])) for i in range(wide)]

        def compute(n, slot):
            at = pl.ds(pl.multiple_of((first + n) * NB, 128), wide * 128)
            qkv[:, at] = jnp.dot(nv[...], wbuf[slot, :, : wide * 128], preferred_element_type=f32).astype(bf16)

        return Phase(count, copies, compute, None, middle)

    def queries(c, middle=None):
        full, rest = divmod(3 * heads, per_tile)
        phases = [qkv_phase(c, 0, full, per_tile, middle)] + ([qkv_phase(c, full, 1, rest)] if rest else [])

        def piece(o, sem, source):
            return pltpu.make_async_copy(source, rv.at[rows_of(o), :], sem)

        def prepare():
            own = piece(z, ls.at[0], x.at[c])
            own.start()
            before = [(None, own, z)]
            for hop in range(LINE):
                now = []
                if hop < LINE - 1:
                    for d in range(2):
                        origin = jnp.clip(line.origin(d, hop + 1), 0, LINE - 1)
                        now.append((line.receives(d, hop), piece(origin, ls.at[1 + d * (LINE - 1) + hop], r.at[c, origin]), origin))
                        xg.settle(d, c, hop)
                        pl.when(now[-1][0])(now[-1][1].start)
                for there, copy, origin in before:
                    def finish():
                        copy.wait()
                        normalize(rv, nv, v["gains"].at[b, pl.ds(0, 1)], v["biases"].at[b, pl.ds(0, 1)], origin * rows, rows)

                    finish() if there is None else pl.when(there)(finish)
                before = now

        run_phases(phases, prepare)

    def attend(c):
        if step:
            key = lambda t: t // rows * step + t % step
            mask = key(lax.broadcasted_iota(jnp.int32, (tokens, tokens), 0)) == key(lax.broadcasted_iota(jnp.int32, (tokens, tokens), 1))

        def head(h, _):
            at = lambda i: pl.ds(pl.multiple_of((i * heads + h) * 128, 128), 128)
            s = lax.dot_general(qkv[:, at(0)], qkv[:, at(1)], (((1,), (1,)), ((), ())), preferred_element_type=f32) * 128**-0.5
            if step:
                s = jnp.where(mask, s, -1e30)
            e = jnp.exp(s - jnp.max(s, axis=-1, keepdims=True))
            p = (e * (1.0 / jnp.sum(e, axis=-1, keepdims=True))).astype(bf16)
            ov[:, pl.ds(pl.multiple_of(h * 128, 128), 128)] = jnp.dot(p, qkv[:, at(2)], preferred_element_type=f32).astype(bf16)
            return 0

        lax.fori_loop(0, heads, head, 0)
        out = pltpu.make_async_copy(ov, o.at[c], ls.at[LINE])
        out.start()
        out.wait()

    def load_o(c):
        both = []
        for s in range(LINE):
            there = nv.at[:, pl.ds(s * hk, hk)]
            both.append((z == s, pltpu.make_async_copy(o.at[c], there, ls.at[s]), pltpu.make_async_copy(og.at[c, s], there, ls.at[s])))
        for own, a, other in both:
            pl.when(own)(a.start)
            pl.when(jnp.logical_not(own))(other.start)
        for _, a, _ in both:
            a.wait()

    def out_phase(c, after, middle):
        def copies(n, slot):
            result = []
            for s in range(LINE):
                there = wbuf.at[slot, pl.ds(s * hk, hk), :]
                result.append((pl.when(z == s), pltpu.make_async_copy(wo.at[b, :, columns(n)], there, ts.at[slot, s])))
                result.append((pl.when(z != s), pltpu.make_async_copy(wg.at[s, :, columns(n)], there, ts.at[slot, s])))
            return result

        def compute(n, slot):
            a = jnp.dot(nv[...], wbuf[slot], preferred_element_type=f32).astype(bf16)
            rv[:, columns(n)] = (rv[:, columns(n)].astype(f32) + a.astype(f32)).astype(bf16)

        return Phase(width // NB, copies, compute, after, middle)

    def up_phase(first, count, wide, after=None):
        cols = lambda n: pl.ds(pl.multiple_of((first + n) * NB, 128), wide)

        def copies(n, slot):
            return [(None, pltpu.make_async_copy(wu.at[b, :, cols(n)], wbuf.at[slot, :, pl.ds(0, wide)], ts.at[slot, 0]))]

        def compute(n, slot):
            u = jnp.dot(nv[...], wbuf[slot, :, :wide], preferred_element_type=f32).astype(bf16).astype(f32)
            gv[:, cols(n)] = jax.nn.gelu(u, approximate=True).astype(bf16)

        return Phase(count, copies, compute, after)

    def down_phase(c, middle):
        count = width // NB

        def store(n, slot):
            return pltpu.make_async_copy(pst.at[slot], part.at[c, :, columns(n)], ds.at[slot])

        def copies(n, slot):
            return [(None, pltpu.make_async_copy(wd.at[b, :, columns(n)], wbuf.at[slot, pl.ds(0, hidden), :], ts.at[slot, 0]))]

        def compute(n, slot):
            s = lax.rem(n, 2)

            @pl.when(n >= 2)
            def _():
                store(n - 2, s).wait()

            pst[s] = jnp.dot(gv[...], wbuf[slot, :hidden, :], preferred_element_type=f32)
            store(n, s).start()

        def after():
            for n in range(max(count - 2, 0), count):
                store(n, n % 2).wait()

        return Phase(count, copies, compute, after, middle)

    def feed(c, mid_out=None, after_out=None, after_up=None, mid_down=None):
        full, rest = divmod(hidden, NB)

        def prepare():
            load_r(c)
            load_o(c)

        def out_done():
            normalize(rv, nv, v["gains"].at[b, pl.ds(1, 1)], v["biases"].at[b, pl.ds(1, 1)], 0, tokens)
            mine[c] = rv[rows_of(z), :]
            if after_out:
                after_out()

        phases = [out_phase(c, out_done, mid_out), up_phase(0, full, NB, None if rest else after_up)]
        if rest:
            phases.append(up_phase(full, 1, rest, after_up))
        run_phases(phases + [down_phase(c, mid_down)], prepare)

    def term(c, t):
        return part.at[c, rows_of(t), :]

    def slot_of(d, c, far):
        return far_got.at[c] if far == LINE - 1 else got.at[d, c, LINE - 2 - far]

    def hop_copy(d, c, far, src):
        return remote(src, slot_of(d, c, far), rs.at[d, c, LINE - 1 - far], rr.at[d, c, LINE - 1 - far], line.target(d))

    def first(d):
        return z == 0 if d == 0 else z == LINE - 1

    def far_target(d, far):
        return z + far if d == 0 else z - far

    half = width // 2
    early = width // NB // 2 + 1 < width // NB

    def early_copy(d):
        cols = pl.ds(0, half)
        src = part.at[0, rows_of(LINE - 1 if d == 0 else 0), cols]
        return remote(src, far_got.at[0, :, cols], v["hs"].at[d], v["hr"].at[d], line.target(d))

    def rest_copy(d):
        cols = pl.ds(half, half)
        src = part.at[0, rows_of(LINE - 1 if d == 0 else 0), cols]
        return remote(src, far_got.at[0, :, cols], rs.at[d, 0, 0], rr.at[d, 0, 0], line.target(d))

    def split(c, far):
        return early and c == 0 and far == LINE - 1

    def reduce_early():
        for d in range(2):
            pl.when(first(d))(lambda: early_copy(d).start())

    def reduce_start(c, fars):
        for far in fars:
            for d in range(2):
                @pl.when(first(d))
                def _():
                    copy = rest_copy(d) if split(c, far) else hop_copy(d, c, far, term(c, far if d == 0 else LINE - 1 - far))
                    copy.start()

    def middle(d, far):
        t = far_target(d, far - 1)
        return jnp.logical_and(jnp.logical_not(first(d)), jnp.logical_and(t >= 0, t < LINE))

    def reduce_relay(c, far):
        for d in range(2):
            @pl.when(middle(d, far))
            def _():
                t = jnp.clip(far_target(d, far - 1), 0, LINE - 1)
                fetch = pltpu.make_async_copy(term(c, t), add, ls.at[LINE + 1])
                fetch.start()
                slot = slot_of(d, c, far)
                if split(c, far):
                    early_copy(d).wait_recv()
                    rest_copy(d).wait_recv()
                else:
                    hop_copy(d, c, far, slot).wait_recv()
                fetch.wait()

                def some(i, _):
                    at = pl.ds(pl.multiple_of(i * RB, RB), RB)
                    slot[at, :] = slot[at, :] + add[at, :]
                    return 0

                lax.fori_loop(0, rows // RB, some, 0)
                hop_copy(d, c, far - 1, slot).start()

    part_rows = rows // 4
    sp = lax.axis_index("sp")

    def turn(c, k):
        device = shift((CORE, Y, Y_CORE)[k])
        there = mine.at[c, pl.ds(pl.multiple_of(device["sp"] * part_rows, part_rows), part_rows), :]
        return remote(there, turned.at[sp * 4 + c], vs.at[c, k], vr.at[c, k], device)

    def turn_own(c):
        return pltpu.make_async_copy(mine.at[c, pl.ds(pl.multiple_of(sp * part_rows, part_rows), part_rows), :], turned.at[sp * 4 + c], ds.at[2 + c])

    def turn_arrive(c, k):
        device = shift((CORE, Y, Y_CORE)[k])
        here = turned.at[device["sp"] * 4 + c]
        remote(here, here, vs.at[c, k], vr.at[c, k], device).wait_recv()

    def reduce_finish(c):
        fetch = pltpu.make_async_copy(term(c, z), add, ls.at[LINE + 1])
        fetch.start()
        for d in range(2):
            @pl.when(jnp.logical_not(first(d)))
            def _():
                hop_copy(d, c, 1, slot_of(d, c, 1)).wait_recv()
        fetch.wait()

        def some(i, _):
            at = pl.ds(pl.multiple_of(i * RB, RB), RB)
            for d in range(2):
                @pl.when(jnp.logical_not(first(d)))
                def _():
                    add[at, :] = add[at, :] + got[d, c, LINE - 3, at, :]
            m = add[at, :].astype(bf16)
            mine[c, at, :] = (mine[c, at, :].astype(f32) + m.astype(f32)).astype(bf16)
            return 0

        lax.fori_loop(0, rows // RB, some, 0)
        turn_own(c).start()
        for k in range(3):
            turn(c, k).start()

    def reduce_sent(c):
        for far in range(LINE - 1, 0, -1):
            for d in range(2):
                @pl.when(first(d))
                def _():
                    if split(c, far):
                        early_copy(d).wait_send()
                        rest_copy(d).wait_send()
                    else:
                        hop_copy(d, c, far, term(c, 0)).wait_send()
                if far > 1:
                    @pl.when(middle(d, far))
                    def _():
                        hop_copy(d, c, far - 1, slot_of(d, c, far)).wait_send()

    outward = lambda d: z == (LINE - 2 if d == 0 else 1)
    inward = lambda d: jnp.logical_not(outward(d))
    inner = lambda d: jnp.logical_and(z > 0, z < LINE - 1)
    outer = lambda d: jnp.logical_not(inner(d))
    both = lambda p, q: (lambda d: jnp.logical_and(p(d), q(d)))

    def later(function):
        return lambda *args, **hooks: functools.partial(function, *args, **hooks)

    def hook(*actions):
        def run():
            for action in actions:
                action()

        return run

    c0, c1, c2, c3 = h0, h1, h2, h3 = range(LINE)
    outwards = (h3, h2, h1)
    XS, XR, OS, OR, OA = later(xg.start), later(xg.relay), later(og_.start), later(og_.relay), later(og_.arrive)
    Q, A, B = later(queries), later(attend), later(feed)
    RS, RR, F = later(reduce_start), later(reduce_relay), later(reduce_finish)
    early_half = reduce_early if early else hook()
    VS, VR = later(w1.along.start), later(w1.along.relay)
    VP, VF, VD = later(w1.spread), later(w1.forward), later(w1.forward_diagonal)

    if b == 0:
        US, UR, UP, UF, UD = (later(f) for f in (w0.along.start, w0.along.relay, w0.spread, w0.forward, w0.forward_diagonal))
        lead = [US(c0, h0), UR(c0, h1), UP(h0), UR(c0, h2), XS(c0, h0), VS(c0, h0, first), XR(c0, h1), VS(c0, h0, both(inner, inward))]
        lead += [UP(h1), UF(h0), UP(h2), XR(c0, h2), XS(c1, h0), XR(c1, h1)]
        after_a0, after_q1, after_a1 = [UD(h0), UF(h1), UF(h2)], [UD(h1)], [UD(h2), later(w0.arrive)(range(h3))]
        after_b0, after_b1, after_rr13 = [VP(h0, inner, "always")], [VF(h0, inner)], [VD(h0, inner)]
        in_b2, after_b2 = [VS(c0, h0, both(inner, outward)), VR(c0, h1, outward, False)], [VR(c0, h1, inward, False)]
        tail0 = [VP(h1, inner, "always"), VP(h0, outer)]
        tail1 = [VR(c0, h2, wait=False), VF(h0, outer), VP(h1, outer)]
        tail2 = [VF(h1, inner)]
        tail3 = [VD(h0, outer), VD(h1, inner), VF(h1, outer)]
        last = [VD(h1, outer), later(w1.arrive)(range(h2))] + [later(w1.along.settle)(d, c0, h2) for d in range(h2)]
        last += [later(w0.along.finish)(h1), later(w0.finish)(range(h3)), later(w1.along.finish)(h1), later(w1.finish)(range(h2))]
    else:
        lead = [VP(h2, wait="never"), XS(c0, h0), XR(c0, h1), XR(c0, h2), XS(c1, h0), XR(c1, h1)]
        after_a0, after_q1, after_a1, last = [VF(h2)], [VD(h2)], [later(w1.arrive)((h2,))], [later(w1.finish)((h2,))]
        after_b0 = after_b1 = after_rr13 = in_b2 = after_b2 = tail0 = tail1 = tail2 = tail3 = []
    schedule = lead + [Q(c0, middle=XR(c1, h2)), A(c0), OS(c0, h0)] + after_a0 + [OR(c0, h1), Q(c1, middle=OR(c0, h2)), XS(c2, h0)] + after_q1
    schedule += [A(c1)] + after_a1 + [OA(c0)]
    schedule += [B(c0, mid_out=XR(c2, h1), after_out=XR(c2, h2), after_up=hook(OS(c1, h0), XS(c3, h0)), mid_down=early_half), RS(c0, outwards), OR(c1, h1)]
    schedule += after_b0 + [Q(c2, middle=hook(OR(c1, h2), XR(c3, h1))), A(c2), OA(c1)]
    schedule += [B(c1, mid_out=RR(c0, h3), after_out=XR(c3, h2), after_up=hook(OS(c2, h0), RR(c0, h2))), RS(c1, outwards[:1])] + after_b1
    schedule += [Q(c3, middle=hook(OR(c2, h1), F(c0))), OR(c2, h2), A(c3), OS(c3, h0), RS(c1, outwards[1:]), RR(c1, h3)] + after_rr13 + [OA(c2)]
    schedule += [B(c2, mid_out=OR(c3, h1), after_out=OR(c3, h2), after_up=hook(RR(c1, h2), *in_b2)), RS(c2, outwards)] + after_b2 + [OA(c3)]
    schedule += [B(c3, after_out=F(c1), after_up=RR(c2, h3)), RS(c3, outwards)] + tail0 + [RR(c2, h2)] + tail1 + [F(c2)] + tail2
    schedule += [RR(c3, h3)] + tail3 + [RR(c3, h2), F(c3)] + last
    meet(line, (CORE, Y, X, Y_CORE))
    for action in schedule:
        action()
    xg.finish(chunks)
    og_.finish(chunks)
    for c in range(chunks):
        reduce_sent(c)
        turn_own(c).wait()
        for k in range(3):
            turn(c, k).wait_send()
            turn_arrive(c, k)


ANY = pl.BlockSpec(memory_space=pl.ANY)
VMEM = pl.BlockSpec(memory_space=pltpu.VMEM)
DMA = pltpu.SemaphoreType.DMA


def call_block(b, step, x, gains, biases, wq, wo, wu, wd, wg):
    chunks, rows, width = x.shape
    hk, tokens, hidden = wo.shape[1], rows * LINE, wu.shape[2]
    hops = LINE - 1
    shape = jax.ShapeDtypeStruct
    outs = [shape((4 * chunks, rows // 4, width), bf16), shape((chunks, LINE, rows, width), bf16), shape((chunks, LINE, tokens, hk), bf16)]
    outs += [shape((chunks, tokens, hk), bf16), shape((chunks, tokens, width), f32)]
    line_sems = DMA((2, chunks, hops))
    scratch = [
        pltpu.VMEM((tokens, width), bf16), pltpu.VMEM((tokens, width), bf16), pltpu.VMEM((tokens, 3 * hk), bf16), pltpu.VMEM((tokens, hk), bf16),
        pltpu.VMEM((tokens, hidden), bf16), pltpu.VMEM((chunks, rows, width), bf16), pltpu.VMEM((SLOTS, width, NB), bf16),
        pltpu.VMEM((chunks, rows, width), f32), pltpu.VMEM((2, chunks, 2, rows, width), f32), pltpu.VMEM((rows, width), f32), pltpu.VMEM((2, tokens, NB), f32),
        line_sems, line_sems, line_sems, line_sems, line_sems, line_sems, DMA((chunks, 3)), DMA((chunks, 3)), DMA((2 * LINE,)), DMA((SLOTS, LINE)), DMA((2 + chunks,)), DMA((2,)), DMA((2,)),
    ]
    outs += [shape((LINE, hk, width), bf16)] * (2 - b)
    scratch += [DMA((2, 2, 1, hops)), DMA((2, 2, 1, hops)), DMA((2, 2, hops, 4)), DMA((2, 2, hops, 4)), DMA((2, 2, hops, 3)), DMA((2, 2, hops, 3))]
    args = [x, gains, biases, wq, wo, wu, wd] + ([] if b == 0 else [wg])
    results = pl.pallas_call(
        functools.partial(block_kernel, b, step),
        out_shape=tuple(outs),
        in_specs=[ANY, VMEM, VMEM] + [ANY] * (len(args) - 3),
        out_specs=tuple(ANY for _ in outs),
        scratch_shapes=scratch,
        input_output_aliases={} if b == 0 else {len(args) - 1: len(outs) - 1},
        compiler_params=pltpu.CompilerParams(collective_id=b, has_side_effects=True, vmem_limit_bytes=VMEM_LIMIT),
        name=f"block_{b}",
    )(*args)
    return results[0], results[-1]


def reorder(a, sizes, order):
    n = a.shape[0] * a.shape[1]
    source = jnp.arange(n).reshape(sizes).transpose(order).reshape(n, 1)
    one_hot = (source == jnp.arange(n)[None]).astype(a.dtype)
    return jnp.dot(one_hot, a.reshape(n, -1), preferred_element_type=f32).astype(a.dtype)


def solution(mesh):
    act_spec = P("data", "sp", "tp", None)
    weight_specs = (P(), P(), P(None, None, None, "tp", None), P(None, "tp", None, None), P(None, None, "tp"), P(None, "tp", None))

    def device_program(x, ln_gain, ln_bias, w_qkv, w_out, w_up, w_down):
        _, frames, rows, width = x.shape
        wq = w_qkv.transpose(0, 2, 3, 1, 4).reshape(2, -1, width, 128)
        wo = w_out.reshape(2, -1, width)
        per = rows // 4
        step = per // 4

        def block(b, r, wg):
            return call_block(b, step if b else 0, r, ln_gain, ln_bias, wq, wo, w_up, w_down, wg)

        spatial, wg = block(0, x[0], None)
        turned = reorder(spatial, (4 * frames, 4, step), (1, 0, 2)).reshape(4, -1, width)
        temporal, _ = block(1, turned, wg)
        return reorder(temporal, (4, 4, frames, step), (2, 0, 1, 3)).reshape(1, frames, rows, width)

    return jax.shard_map(device_program, mesh=mesh, in_specs=(act_spec,) + weight_specs, out_specs=act_spec, check_vma=False)
```

```python
import functools

import jax
import jax.numpy as jnp
from jax import lax
from jax.experimental import pallas as pl
from jax.experimental.pallas import tpu as pltpu
from jax.sharding import PartitionSpec as P

bf16, f32 = jnp.bfloat16, jnp.float32
MESH = pl.DeviceIdType.MESH
LINE = 4
NB = 512
SLOTS = 3
RB = 16
LN_ROWS = 64
VMEM_LIMIT = 66_500_000


CORE, Y, X, Y_CORE = (0, 0, 1), (0, 1, 0), (1, 0, 0), (0, 1, 1)


def shift(flips):
    data, sp = lax.axis_index("data"), lax.axis_index("sp")
    y, core = sp // 2, sp % 2
    return {"data": 1 - data if flips[0] else data, "sp": (1 - y if flips[1] else y) * 2 + (1 - core if flips[2] else core)}


def place_of(device):
    return device["data"] * 4 + device["sp"]


ARRIVALS = (((1, 0), (0, 0), (0, 0), (0, 0)), ((1, 1), (1, 0), (1, 0), (0, 1)), ((1, 2), (1, 1), (0, 1), (0, 2)))


class Line:
    def __init__(self):
        self.z = lax.axis_index("tp")

    def exists(self, direction):
        return self.z < LINE - 1 if direction == 0 else self.z > 0

    def source_exists(self, direction):
        return self.z > 0 if direction == 0 else self.z < LINE - 1

    def target(self, direction):
        return {"tp": self.z + 1 if direction == 0 else self.z - 1}

    def origin(self, direction, hop):
        return self.z - hop if direction == 0 else self.z + hop

    def sends(self, direction, hop):
        o = self.origin(direction, hop)
        return jnp.logical_and(self.exists(direction), jnp.logical_and(o >= 0, o < LINE))

    def receives(self, direction, hop):
        o = self.origin(direction, hop + 1)
        return jnp.logical_and(o >= 0, o < LINE)


def remote(src, dst, send, recv, device):
    return pltpu.make_async_remote_copy(src_ref=src, dst_ref=dst, send_sem=send, recv_sem=recv, device_id=device, device_id_type=MESH)


class Gather:
    def __init__(self, line, own, slot, send, recv):
        self.line, self.own, self.slot, self.send, self.recv = line, own, slot, send, recv

    def copy(self, d, c, hop):
        o = jnp.clip(self.line.origin(d, hop), 0, LINE - 1)
        src = self.own(c) if hop == 0 else self.slot(c, o)
        return remote(src, self.slot(c, o), self.send.at[d, c, hop], self.recv.at[d, c, hop], self.line.target(d))

    def arrival(self, d, c, hop):
        o = jnp.clip(self.line.origin(d, hop + 1), 0, LINE - 1)
        here = self.slot(c, o)
        return remote(here, here, self.send.at[d, c, hop], self.recv.at[d, c, hop], self.line.target(d))

    def start(self, c, hop, only=lambda d: True):
        for d in range(2):
            @pl.when(jnp.logical_and(self.line.sends(d, hop), only(d)))
            def _():
                self.copy(d, c, hop).start()

    def arrive(self, c):
        for hop in range(LINE - 1):
            for d in range(2):
                self.settle(d, c, hop)

    def settle(self, d, c, hop):
        passed_on = self.line.sends(d, hop + 1) if hop + 1 < LINE - 1 else False

        @pl.when(jnp.logical_and(self.line.receives(d, hop), jnp.logical_not(passed_on)))
        def _():
            self.arrival(d, c, hop).wait_recv()

    def relay(self, c, hop, only=lambda d: True, wait=True):
        for d in range(2):
            @pl.when(jnp.logical_and(self.line.sends(d, hop), only(d)))
            def _():
                if wait:
                    self.arrival(d, c, hop - 1).wait_recv()
                self.copy(d, c, hop).start()

    def finish(self, chunks):
        for c in range(chunks):
            for hop in range(LINE - 1):
                for d in range(2):
                    @pl.when(self.line.sends(d, hop))
                    def _():
                        self.copy(d, c, hop).wait_send()


def meet(line, peers):
    barrier = pltpu.get_barrier_semaphore()
    for d in range(2):
        @pl.when(line.exists(d))
        def _():
            pl.semaphore_signal(barrier, inc=1, device_id=line.target(d), device_id_type=MESH)
    for p in peers:
        pl.semaphore_signal(barrier, inc=1, device_id=shift(p), device_id_type=MESH)
    pl.semaphore_wait(barrier, jnp.where(jnp.logical_or(line.z == 0, line.z == LINE - 1), 1, 2) + len(peers))


def normalize(src, dst, gain, bias, start, count):
    block = min(count, LN_ROWS)

    def some(i, _):
        at = pl.ds(pl.multiple_of(start + i * block, RB), block)
        u = src[at, :].astype(f32)
        u = u - jnp.mean(u, axis=-1, keepdims=True)
        var = jnp.mean(u * u, axis=-1, keepdims=True)
        dst[at, :] = (u * lax.rsqrt(var + 1e-6) * gain[...] + bias[...]).astype(bf16)
        return 0

    lax.fori_loop(0, count // block, some, 0)


class Phase:
    def __init__(self, count, copies, compute, after=None, middle=None, before=None):
        self.count, self.copies, self.compute, self.after, self.middle, self.before = count, copies, compute, after, middle, before

    def start(self, n, slot):
        for when, copy in self.copies(n, slot):
            when(copy.start) if when else copy.start()

    def wait(self, n, slot):
        for when, copy in self.copies(n, slot):
            when(copy.wait) if when else copy.wait()


def run_phases(phases, prepare):
    flat = [(p, n) for p in phases for n in range(p.count)]
    ahead = SLOTS - 1
    for i in range(ahead):
        flat[i][0].start(flat[i][1], i)
    prepare()
    base = 0
    for p in phases:
        later = flat[base + p.count : base + p.count + ahead]

        def step(n, _):
            slot = lax.rem(base + n, SLOTS)
            if p.count > ahead:
                @pl.when(n + ahead < p.count)
                def _():
                    p.start(n + ahead, lax.rem(base + n + ahead, SLOTS))
            for j, (q, m) in enumerate(later):
                when = p.count + j - ahead
                if when >= 0:
                    @pl.when(n == when)
                    def _():
                        q.start(m, (base + p.count + j) % SLOTS)
            p.wait(n, slot)
            p.compute(n, slot)
            if p.middle:
                pl.when(n == min(p.count // 2 + 1, p.count - 1))(p.middle)
            return 0

        if p.before:
            p.before()
        if p.count == 1:
            step(0, 0)
        else:
            lax.fori_loop(0, p.count, step, 0)
        if p.after:
            p.after()
        base += p.count


class PlaneGather:
    def __init__(self, line, own, wg, ws, wr, ps, pr, fs, fr):
        width = wg.shape[2]
        cols = width // 8
        self.line, self.wg, self.ps, self.pr, self.fs, self.fr = line, wg, ps, pr, fs, fr
        self.cols = lambda p: pl.ds(pl.multiple_of(p * cols, 128), cols)
        me = shift((0, 0, 0))
        self.place = place_of(me)
        self.core = lax.axis_index("sp") % 2
        self.along = Gather(line, lambda c: own.at[:, self.cols(self.place)], lambda c, o: wg.at[o, :, self.cols(self.place)], ws, wr)
        across, beside = shift(X), shift(Y)
        first_is_x = self.core == 0
        self.diagonal_device = {k: jnp.where(first_is_x, beside[k], across[k]) for k in across}
        self.diagonal_given = jnp.where(first_is_x, place_of(across), place_of(beside))
        self.sources = (place_of(shift(CORE)), place_of(beside), place_of(across), place_of(shift((1, 1, 0))))

    def each(self, hop, action, only=lambda d: True):
        for d in range(2):
            @pl.when(jnp.logical_and(self.line.receives(d, hop), only(d)))
            def _():
                o = jnp.clip(self.line.origin(d, hop + 1), 0, LINE - 1)
                action(d, lambda p: self.wg.at[o, :, self.cols(p)])

    def direct(self, d, hop, k, ref):
        return remote(ref, ref, self.ps.at[d, hop, k], self.pr.at[d, hop, k], shift((CORE, Y, X)[k]))

    def diagonal(self, d, hop, ref):
        return remote(ref, ref, self.ps.at[d, hop, 3], self.pr.at[d, hop, 3], self.diagonal_device)

    def pass_on(self, d, hop, k, ref):
        return remote(ref, ref, self.fs.at[d, hop, k - 1], self.fr.at[d, hop, k - 1], shift(CORE))

    def spread(self, hop, only=lambda d: True, wait="unless relayed"):
        def action(d, slab):
            if wait == "always":
                self.along.arrival(d, 0, hop).wait_recv()
            elif wait == "unless relayed":
                self.along.settle(d, 0, hop)
            for k in range(3):
                self.direct(d, hop, k, slab(self.place)).start()

        self.each(hop, action, only)

    def forward(self, hop, only=lambda d: True):
        def action(d, slab):
            for k in (1, 2):
                self.direct(d, hop, k, slab(self.sources[k])).wait_recv()
                self.pass_on(d, hop, k, slab(self.sources[k])).start()
            self.diagonal(d, hop, slab(self.diagonal_given)).start()

        self.each(hop, action, only)

    def forward_diagonal(self, hop, only=lambda d: True):
        def action(d, slab):
            self.diagonal(d, hop, slab(self.sources[3])).wait_recv()
            self.pass_on(d, hop, 3, slab(self.sources[3])).start()

        self.each(hop, action, only)

    def arrive(self, hops):
        for hop in hops:
            def action(d, slab):
                self.direct(d, hop, 0, slab(self.sources[0])).wait_recv()
                for k in (1, 2, 3):
                    p = self.sources[k]
                    self.pass_on(d, hop, k, slab(p + 1 - 2 * (p % 2))).wait_recv()

            self.each(hop, action)

    def finish(self, hops):
        for hop in hops:
            def action(d, slab):
                for k in range(3):
                    self.direct(d, hop, k, slab(self.place)).wait_send()
                self.diagonal(d, hop, slab(self.diagonal_given)).wait_send()
                for k in (1, 2, 3):
                    self.pass_on(d, hop, k, slab(self.sources[k])).wait_send()

            self.each(hop, action)


def block_kernel(b, step, *refs):
    names = ["x", "gains", "biases", "wq", "wo", "wu", "wd"] + ([] if b == 0 else ["wg_in"])
    names += ["turned", "r", "og", "o", "part"] + (["wg0", "wg1"] if b == 0 else ["wg1"])
    scratch_names = ["rv", "nv", "qkv", "ov", "gv", "mine", "acc", "wbuf", "far_got", "got", "add", "pst"]
    names += scratch_names
    names += ["xs", "xr", "os", "or_", "rs", "rr", "vs", "vr", "ls", "ts", "ds", "hs", "hr", "ws", "wr", "ps", "pr", "fs", "fr"]
    v = dict(zip(names, refs, strict=True))
    x, r, o, og, part, turned = (v[k] for k in ("x", "r", "o", "og", "part", "turned"))
    wq, wo, wu, wd = (v[k] for k in ("wq", "wo", "wu", "wd"))
    rv, nv, qkv, ov, gv, mine, acc, wbuf, far_got, got, add, pst = (v[k] for k in scratch_names)
    rs, rr, vs, vr, ls, ts, ds = (v[k] for k in ("rs", "rr", "vs", "vr", "ls", "ts", "ds"))
    wg = v[f"wg{b}"]
    chunks, rows, width = x.shape
    tokens = rows * LINE
    hk, hidden = wo.shape[1], wu.shape[2]
    heads = hk // 128
    line = Line()
    z = line.z
    xg = Gather(line, lambda c: x.at[c], lambda c, s: r.at[c, s], v["xs"], v["xr"])
    og_ = Gather(line, lambda c: o.at[c], lambda c, s: og.at[c, s], v["os"], v["or_"])
    w0, w1 = (PlaneGather(line, wo.at[i], v[f"wg{i}"], *(v[k].at[i] for k in ("ws", "wr", "ps", "pr", "fs", "fr"))) if i >= b else None for i in range(2))

    def rows_of(o):
        return pl.ds(pl.multiple_of(o * rows, rows), rows)

    def columns(n):
        return pl.ds(pl.multiple_of(n * NB, 128), NB)

    def r_copies(c, own=True):
        return [pltpu.make_async_copy(x.at[c] if own else r.at[c, s], rv.at[rows_of(s), :], ls.at[s]) for s in range(LINE)]

    def load_r(c):
        for s, (a, other) in enumerate(zip(r_copies(c), r_copies(c, False))):
            pl.when(z == s)(a.start)
            pl.when(z != s)(other.start)

    per_tile = NB // 128

    def qkv_phase(c, first, count, wide, middle=None):
        def copies(n, slot):
            return [(None, pltpu.make_async_copy(wq.at[b, (first + n) * per_tile + i], wbuf.at[slot, :, pl.ds(i * 128, 128)], ts.at[slot, i])) for i in range(wide)]

        def compute(n, slot):
            at = pl.ds(pl.multiple_of((first + n) * NB, 128), wide * 128)
            qkv[:, at] = jnp.dot(nv[...], wbuf[slot, :, : wide * 128], preferred_element_type=f32).astype(bf16)

        return Phase(count, copies, compute, None, middle)

    def queries(c, middle=None):
        full, rest = divmod(3 * heads, per_tile)
        phases = [qkv_phase(c, 0, full, per_tile, middle)] + ([qkv_phase(c, full, 1, rest)] if rest else [])

        def piece(o, sem, source):
            return pltpu.make_async_copy(source, rv.at[rows_of(o), :], sem)

        def prepare():
            own = piece(z, ls.at[0], x.at[c])
            own.start()
            before = [(None, own, z)]
            for hop in range(LINE):
                now = []
                if hop < LINE - 1:
                    for d in range(2):
                        origin = jnp.clip(line.origin(d, hop + 1), 0, LINE - 1)
                        now.append((line.receives(d, hop), piece(origin, ls.at[1 + d * (LINE - 1) + hop], r.at[c, origin]), origin))
                        xg.settle(d, c, hop)
                        pl.when(now[-1][0])(now[-1][1].start)
                for there, copy, origin in before:
                    def finish():
                        copy.wait()
                        normalize(rv, nv, v["gains"].at[b, pl.ds(0, 1)], v["biases"].at[b, pl.ds(0, 1)], origin * rows, rows)

                    finish() if there is None else pl.when(there)(finish)
                before = now

        run_phases(phases, prepare)

    def attend(c):
        if step:
            key = lambda t: t // rows * step + t % step
            mask = key(lax.broadcasted_iota(jnp.int32, (tokens, tokens), 0)) == key(lax.broadcasted_iota(jnp.int32, (tokens, tokens), 1))

        def head(h, _):
            at = lambda i: pl.ds(pl.multiple_of((i * heads + h) * 128, 128), 128)
            s = lax.dot_general(qkv[:, at(0)], qkv[:, at(1)], (((1,), (1,)), ((), ())), preferred_element_type=f32) * 128**-0.5
            if step:
                s = jnp.where(mask, s, -1e30)
            e = jnp.exp(s - jnp.max(s, axis=-1, keepdims=True))
            p = (e * (1.0 / jnp.sum(e, axis=-1, keepdims=True))).astype(bf16)
            ov[:, pl.ds(pl.multiple_of(h * 128, 128), 128)] = jnp.dot(p, qkv[:, at(2)], preferred_element_type=f32).astype(bf16)
            return 0

        lax.fori_loop(0, heads, head, 0)
        out = pltpu.make_async_copy(ov, o.at[c], ls.at[2 * LINE])
        out.start()
        out.wait()

    def block_of(i):
        origins = [zz + (hop + 1 if d else -hop - 1) for zz, (d, hop) in enumerate(ARRIVALS[i - 1])]
        return functools.reduce(lambda rest, zz: jnp.where(z == zz, origins[zz], rest), range(LINE), 0)

    def fetch_o(c, i):
        source = o.at[c] if i == 0 else og.at[c, block_of(i)]
        return pltpu.make_async_copy(source, nv.at[:, pl.ds(i * hk, hk)], ls.at[LINE + i])

    def arrive_o(c, i):
        for zz, (d, hop) in enumerate(ARRIVALS[i - 1]):
            pl.when(z == zz)(functools.partial(og_.settle, d, c, hop))
        fetch_o(c, i).start()

    def out_phase(c, i, after):
        wide = 2 if width % (2 * NB) == 0 else 1

        def copies(n, slot):
            source = wo.at[b] if i == 0 else wg.at[block_of(i)]
            return [(None, pltpu.make_async_copy(source.at[:, columns(wide * n + j)], wbuf.at[slot, pl.ds(j * hk, hk), :], ts.at[slot, j])) for j in range(wide)]

        def compute(n, slot):
            for j in range(wide):
                at = columns(wide * n + j)
                a = jnp.dot(nv[:, i * hk : (i + 1) * hk], wbuf[slot, j * hk : (j + 1) * hk, :], preferred_element_type=f32)
                if i > 0:
                    a = acc[:, at] + a
                if i < LINE - 1:
                    acc[:, at] = a
                else:
                    rv[:, at] = (rv[:, at].astype(f32) + a.astype(bf16).astype(f32)).astype(bf16)

        def before():
            fetch_o(c, i).wait()
            if i == LINE - 1:
                for copy in r_copies(c):
                    copy.wait()

        middle = functools.partial(arrive_o, c, i + 1) if i < LINE - 1 else None
        return Phase(width // (wide * NB), copies, compute, after, middle, before)

    def up_phase(after):
        cols = lambda n: pl.ds(pl.multiple_of(jnp.minimum(n * NB, hidden - NB), 128), NB)

        def copies(n, slot):
            return [(None, pltpu.make_async_copy(wu.at[b, :, cols(n)], wbuf.at[slot], ts.at[slot, 0]))]

        def compute(n, slot):
            u = jnp.dot(nv[...], wbuf[slot], preferred_element_type=f32).astype(bf16).astype(f32)
            gv[:, cols(n)] = jax.nn.gelu(u, approximate=True).astype(bf16)

        return Phase(pl.cdiv(hidden, NB), copies, compute, after)

    def down_phase(c, middle):
        count = width // NB

        def store(n, slot):
            return pltpu.make_async_copy(pst.at[slot], part.at[c, :, columns(n)], ds.at[slot])

        def copies(n, slot):
            return [(None, pltpu.make_async_copy(wd.at[b, :, columns(n)], wbuf.at[slot, pl.ds(0, hidden), :], ts.at[slot, 0]))]

        def compute(n, slot):
            s = lax.rem(n, 2)

            @pl.when(n >= 2)
            def _():
                store(n - 2, s).wait()

            pst[s] = jnp.dot(gv[...], wbuf[slot, :hidden, :], preferred_element_type=f32)
            store(n, s).start()

        def after():
            for n in range(max(count - 2, 0), count):
                store(n, n % 2).wait()

        return Phase(count, copies, compute, after, middle)

    def feed(c, mid_out=None, after_out=None, after_up=None, mid_down=None):
        def prepare():
            load_r(c)
            fetch_o(c, 0).start()

        def out_done():
            normalize(rv, nv, v["gains"].at[b, pl.ds(1, 1)], v["biases"].at[b, pl.ds(1, 1)], 0, tokens)
            mine[c] = rv[rows_of(z), :]
            if after_out:
                after_out()

        phases = [out_phase(c, i, after) for i, after in enumerate((None, mid_out, None, out_done))] + [up_phase(after_up)]
        run_phases(phases + [down_phase(c, mid_down)], prepare)

    def term(c, t):
        return part.at[c, rows_of(t), :]

    def slot_of(d, c, far):
        return far_got.at[c] if far == LINE - 1 else got.at[d, c, LINE - 2 - far]

    def hop_copy(d, c, far, src):
        return remote(src, slot_of(d, c, far), rs.at[d, c, LINE - 1 - far], rr.at[d, c, LINE - 1 - far], line.target(d))

    def first(d):
        return z == 0 if d == 0 else z == LINE - 1

    def far_target(d, far):
        return z + far if d == 0 else z - far

    half = width // 2
    early = width // NB // 2 + 1 < width // NB

    def early_copy(d):
        cols = pl.ds(0, half)
        src = part.at[0, rows_of(LINE - 1 if d == 0 else 0), cols]
        return remote(src, far_got.at[0, :, cols], v["hs"].at[d], v["hr"].at[d], line.target(d))

    def rest_copy(d):
        cols = pl.ds(half, half)
        src = part.at[0, rows_of(LINE - 1 if d == 0 else 0), cols]
        return remote(src, far_got.at[0, :, cols], rs.at[d, 0, 0], rr.at[d, 0, 0], line.target(d))

    def split(c, far):
        return early and c == 0 and far == LINE - 1

    def reduce_early():
        for d in range(2):
            pl.when(first(d))(lambda: early_copy(d).start())

    def reduce_start(c, fars):
        for far in fars:
            for d in range(2):
                @pl.when(first(d))
                def _():
                    copy = rest_copy(d) if split(c, far) else hop_copy(d, c, far, term(c, far if d == 0 else LINE - 1 - far))
                    copy.start()

    def middle(d, far):
        t = far_target(d, far - 1)
        return jnp.logical_and(jnp.logical_not(first(d)), jnp.logical_and(t >= 0, t < LINE))

    def reduce_relay(c, far):
        for d in range(2):
            @pl.when(middle(d, far))
            def _():
                t = jnp.clip(far_target(d, far - 1), 0, LINE - 1)
                fetch = pltpu.make_async_copy(term(c, t), add, ls.at[2 * LINE])
                fetch.start()
                slot = slot_of(d, c, far)
                if split(c, far):
                    early_copy(d).wait_recv()
                    rest_copy(d).wait_recv()
                else:
                    hop_copy(d, c, far, slot).wait_recv()
                fetch.wait()

                def some(i, _):
                    at = pl.ds(pl.multiple_of(i * RB, RB), RB)
                    slot[at, :] = slot[at, :] + add[at, :]
                    return 0

                lax.fori_loop(0, rows // RB, some, 0)
                hop_copy(d, c, far - 1, slot).start()

    part_rows = rows // 4
    sp = lax.axis_index("sp")

    def turn(c, k):
        device = shift((CORE, Y, Y_CORE)[k])
        there = mine.at[c, pl.ds(pl.multiple_of(device["sp"] * part_rows, part_rows), part_rows), :]
        return remote(there, turned.at[sp * 4 + c], vs.at[c, k], vr.at[c, k], device)

    def turn_own(c):
        return pltpu.make_async_copy(mine.at[c, pl.ds(pl.multiple_of(sp * part_rows, part_rows), part_rows), :], turned.at[sp * 4 + c], ds.at[2 + c])

    def turn_arrive(c, k):
        device = shift((CORE, Y, Y_CORE)[k])
        here = turned.at[device["sp"] * 4 + c]
        remote(here, here, vs.at[c, k], vr.at[c, k], device).wait_recv()

    def reduce_finish(c):
        fetch = pltpu.make_async_copy(term(c, z), add, ls.at[2 * LINE])
        fetch.start()
        for d in range(2):
            @pl.when(jnp.logical_not(first(d)))
            def _():
                hop_copy(d, c, 1, slot_of(d, c, 1)).wait_recv()
        fetch.wait()

        def some(i, _):
            at = pl.ds(pl.multiple_of(i * RB, RB), RB)
            for d in range(2):
                @pl.when(jnp.logical_not(first(d)))
                def _():
                    add[at, :] = add[at, :] + got[d, c, LINE - 3, at, :]
            m = add[at, :].astype(bf16)
            mine[c, at, :] = (mine[c, at, :].astype(f32) + m.astype(f32)).astype(bf16)
            return 0

        lax.fori_loop(0, rows // RB, some, 0)
        turn_own(c).start()
        for k in range(3):
            turn(c, k).start()

    def reduce_sent(c):
        for far in range(LINE - 1, 0, -1):
            for d in range(2):
                @pl.when(first(d))
                def _():
                    if split(c, far):
                        early_copy(d).wait_send()
                        rest_copy(d).wait_send()
                    else:
                        hop_copy(d, c, far, term(c, 0)).wait_send()
                if far > 1:
                    @pl.when(middle(d, far))
                    def _():
                        hop_copy(d, c, far - 1, slot_of(d, c, far)).wait_send()

    outward = lambda d: z == (LINE - 2 if d == 0 else 1)
    inward = lambda d: jnp.logical_not(outward(d))
    inner = lambda d: jnp.logical_and(z > 0, z < LINE - 1)
    outer = lambda d: jnp.logical_not(inner(d))
    both = lambda p, q: (lambda d: jnp.logical_and(p(d), q(d)))

    def later(function):
        return lambda *args, **hooks: functools.partial(function, *args, **hooks)

    def hook(*actions):
        def run():
            for action in actions:
                action()

        return run

    c0, c1, c2, c3 = h0, h1, h2, h3 = range(LINE)
    outwards = (h3, h2, h1)
    XS, XR, OS, OR = later(xg.start), later(xg.relay), later(og_.start), later(og_.relay)
    Q, A, B = later(queries), later(attend), later(feed)
    RS, RR, F = later(reduce_start), later(reduce_relay), later(reduce_finish)
    early_half = reduce_early if early else hook()
    VS, VR = later(w1.along.start), later(w1.along.relay)
    VP, VF, VD = later(w1.spread), later(w1.forward), later(w1.forward_diagonal)

    if b == 0:
        US, UR, UP, UF, UD = (later(f) for f in (w0.along.start, w0.along.relay, w0.spread, w0.forward, w0.forward_diagonal))
        lead = [US(c0, h0), UR(c0, h1), UP(h0), UR(c0, h2), XS(c0, h0), VS(c0, h0, first), XR(c0, h1), VS(c0, h0, both(inner, inward))]
        lead += [UP(h1), UF(h0), UP(h2), XR(c0, h2), XS(c1, h0), XR(c1, h1)]
        after_a0, after_q1, after_a1 = [UD(h0), UF(h1), UF(h2)], [UD(h1)], [UD(h2), later(w0.arrive)(range(h3))]
        after_b0, after_b1, after_rr13 = [VP(h0, inner, "always")], [VF(h0, inner)], [VD(h0, inner)]
        in_b2, after_b2 = [VS(c0, h0, both(inner, outward)), VR(c0, h1, outward, False)], [VR(c0, h1, inward, False)]
        tail0 = [VP(h1, inner, "always"), VP(h0, outer)]
        tail1 = [VR(c0, h2, wait=False), VF(h0, outer), VP(h1, outer)]
        tail2 = [VF(h1, inner)]
        tail3 = [VD(h0, outer), VD(h1, inner), VF(h1, outer)]
        last = [VD(h1, outer), later(w1.arrive)(range(h2))] + [later(w1.along.settle)(d, c0, h2) for d in range(h2)]
        last += [later(w0.along.finish)(h1), later(w0.finish)(range(h3)), later(w1.along.finish)(h1), later(w1.finish)(range(h2))]
    else:
        lead = [VP(h2, wait="never"), XS(c0, h0), XR(c0, h1), XR(c0, h2), XS(c1, h0), XR(c1, h1)]
        after_a0, after_q1, after_a1, last = [VF(h2)], [VD(h2)], [later(w1.arrive)((h2,))], [later(w1.finish)((h2,))]
        after_b0 = after_b1 = after_rr13 = in_b2 = after_b2 = tail0 = tail1 = tail2 = tail3 = []
    schedule = lead + [Q(c0, middle=XR(c1, h2)), A(c0), OS(c0, h0)] + after_a0 + [OR(c0, h1), Q(c1, middle=OR(c0, h2)), XS(c2, h0)] + after_q1
    schedule += [A(c1)] + after_a1
    schedule += [B(c0, mid_out=XR(c2, h1), after_out=XR(c2, h2), after_up=hook(OS(c1, h0), XS(c3, h0)), mid_down=early_half), RS(c0, outwards), OR(c1, h1)]
    schedule += after_b0 + [Q(c2, middle=hook(OR(c1, h2), XR(c3, h1))), A(c2)]
    schedule += [B(c1, mid_out=RR(c0, h3), after_out=XR(c3, h2), after_up=hook(OS(c2, h0), RR(c0, h2))), RS(c1, outwards[:1])] + after_b1
    schedule += [Q(c3, middle=hook(OR(c2, h1), F(c0))), OR(c2, h2), A(c3), OS(c3, h0), RS(c1, outwards[1:]), RR(c1, h3)] + after_rr13
    schedule += [B(c2, mid_out=OR(c3, h1), after_out=OR(c3, h2), after_up=hook(RR(c1, h2), *in_b2)), RS(c2, outwards)] + after_b2
    schedule += [B(c3, after_out=F(c1), after_up=RR(c2, h3)), RS(c3, outwards)] + tail0 + [RR(c2, h2)] + tail1 + [F(c2)] + tail2
    schedule += [RR(c3, h3)] + tail3 + [RR(c3, h2), F(c3)] + last
    meet(line, (CORE, Y, X, Y_CORE))
    for action in schedule:
        action()
    xg.finish(chunks)
    og_.finish(chunks)
    for c in range(chunks):
        reduce_sent(c)
        turn_own(c).wait()
        for k in range(3):
            turn(c, k).wait_send()
            turn_arrive(c, k)


ANY = pl.BlockSpec(memory_space=pl.ANY)
VMEM = pl.BlockSpec(memory_space=pltpu.VMEM)
DMA = pltpu.SemaphoreType.DMA


def call_block(b, step, x, gains, biases, wq, wo, wu, wd, wg):
    chunks, rows, width = x.shape
    hk, tokens, hidden = wo.shape[1], rows * LINE, wu.shape[2]
    hops = LINE - 1
    shape = jax.ShapeDtypeStruct
    outs = [shape((4 * chunks, rows // 4, width), bf16), shape((chunks, LINE, rows, width), bf16), shape((chunks, LINE, tokens, hk), bf16)]
    outs += [shape((chunks, tokens, hk), bf16), shape((chunks, tokens, width), f32)]
    line_sems = DMA((2, chunks, hops))
    scratch = [
        pltpu.VMEM((tokens, width), bf16), pltpu.VMEM((tokens, width), bf16), pltpu.VMEM((tokens, 3 * hk), bf16), pltpu.VMEM((tokens, hk), bf16),
        pltpu.VMEM((tokens, hidden), bf16), pltpu.VMEM((chunks, rows, width), bf16), pltpu.VMEM((tokens, width), f32), pltpu.VMEM((SLOTS, width, NB), bf16),
        pltpu.VMEM((chunks, rows, width), f32), pltpu.VMEM((2, chunks, 2, rows, width), f32), pltpu.VMEM((rows, width), f32), pltpu.VMEM((2, tokens, NB), f32),
        line_sems, line_sems, line_sems, line_sems, line_sems, line_sems, DMA((chunks, 3)), DMA((chunks, 3)), DMA((3 * LINE,)), DMA((SLOTS, LINE)), DMA((2 + chunks,)), DMA((2,)), DMA((2,)),
    ]
    outs += [shape((LINE, hk, width), bf16)] * (2 - b)
    scratch += [DMA((2, 2, 1, hops)), DMA((2, 2, 1, hops)), DMA((2, 2, hops, 4)), DMA((2, 2, hops, 4)), DMA((2, 2, hops, 3)), DMA((2, 2, hops, 3))]
    args = [x, gains, biases, wq, wo, wu, wd] + ([] if b == 0 else [wg])
    results = pl.pallas_call(
        functools.partial(block_kernel, b, step),
        out_shape=tuple(outs),
        in_specs=[ANY, VMEM, VMEM] + [ANY] * (len(args) - 3),
        out_specs=tuple(ANY for _ in outs),
        scratch_shapes=scratch,
        input_output_aliases={} if b == 0 else {len(args) - 1: len(outs) - 1},
        compiler_params=pltpu.CompilerParams(collective_id=b, has_side_effects=True, vmem_limit_bytes=VMEM_LIMIT),
        name=f"block_{b}",
    )(*args)
    return results[0], results[-1]


def reorder(a, sizes, order):
    n = a.shape[0] * a.shape[1]
    source = jnp.arange(n).reshape(sizes).transpose(order).reshape(n, 1)
    one_hot = (source == jnp.arange(n)[None]).astype(a.dtype)
    return jnp.dot(one_hot, a.reshape(n, -1), preferred_element_type=f32).astype(a.dtype)


def solution(mesh):
    act_spec = P("data", "sp", "tp", None)
    weight_specs = (P(), P(), P(None, None, None, "tp", None), P(None, "tp", None, None), P(None, None, "tp"), P(None, "tp", None))

    def device_program(x, ln_gain, ln_bias, w_qkv, w_out, w_up, w_down):
        _, frames, rows, width = x.shape
        wq = w_qkv.transpose(0, 2, 3, 1, 4).reshape(2, -1, width, 128)
        wo = w_out.reshape(2, -1, width)
        per = rows // 4
        step = per // 4

        def block(b, r, wg):
            return call_block(b, step if b else 0, r, ln_gain, ln_bias, wq, wo, w_up, w_down, wg)

        spatial, wg = block(0, x[0], None)
        turned = reorder(spatial, (4 * frames, 4, step), (1, 0, 2)).reshape(4, -1, width)
        temporal, _ = block(1, turned, wg)
        return reorder(temporal, (4, 4, frames, step), (2, 0, 1, 3)).reshape(1, frames, rows, width)

    return jax.shard_map(device_program, mesh=mesh, in_specs=(act_spec,) + weight_specs, out_specs=act_spec, check_vma=False)
```

```python
import functools

import jax
import jax.numpy as jnp
from jax import lax
from jax.experimental import pallas as pl
from jax.experimental.pallas import tpu as pltpu
from jax.sharding import PartitionSpec as P

bf16, f32 = jnp.bfloat16, jnp.float32
MESH = pl.DeviceIdType.MESH
LINE = 4
NB = 512
SLOTS = 3
RB = 16
LN_ROWS = 64
VMEM_LIMIT = 66_500_000


CORE, Y, X, Y_CORE = (0, 0, 1), (0, 1, 0), (1, 0, 0), (0, 1, 1)


def shift(flips):
    data, sp = lax.axis_index("data"), lax.axis_index("sp")
    y, core = sp // 2, sp % 2
    return {"data": 1 - data if flips[0] else data, "sp": (1 - y if flips[1] else y) * 2 + (1 - core if flips[2] else core)}


def place_of(device):
    return device["data"] * 4 + device["sp"]


ARRIVALS = (((1, 0), (0, 0), (0, 0), (0, 0)), ((1, 1), (1, 0), (1, 0), (0, 1)), ((1, 2), (1, 1), (0, 1), (0, 2)))


class Line:
    def __init__(self):
        self.z = lax.axis_index("tp")

    def exists(self, direction):
        return self.z < LINE - 1 if direction == 0 else self.z > 0

    def source_exists(self, direction):
        return self.z > 0 if direction == 0 else self.z < LINE - 1

    def target(self, direction):
        return {"tp": self.z + 1 if direction == 0 else self.z - 1}

    def origin(self, direction, hop):
        return self.z - hop if direction == 0 else self.z + hop

    def sends(self, direction, hop):
        o = self.origin(direction, hop)
        return jnp.logical_and(self.exists(direction), jnp.logical_and(o >= 0, o < LINE))

    def receives(self, direction, hop):
        o = self.origin(direction, hop + 1)
        return jnp.logical_and(o >= 0, o < LINE)


def remote(src, dst, send, recv, device):
    return pltpu.make_async_remote_copy(src_ref=src, dst_ref=dst, send_sem=send, recv_sem=recv, device_id=device, device_id_type=MESH)


class Gather:
    def __init__(self, line, own, slot, send, recv):
        self.line, self.own, self.slot, self.send, self.recv = line, own, slot, send, recv

    def copy(self, d, c, hop):
        o = jnp.clip(self.line.origin(d, hop), 0, LINE - 1)
        src = self.own(c) if hop == 0 else self.slot(c, o)
        return remote(src, self.slot(c, o), self.send.at[d, c, hop], self.recv.at[d, c, hop], self.line.target(d))

    def arrival(self, d, c, hop):
        o = jnp.clip(self.line.origin(d, hop + 1), 0, LINE - 1)
        here = self.slot(c, o)
        return remote(here, here, self.send.at[d, c, hop], self.recv.at[d, c, hop], self.line.target(d))

    def start(self, c, hop, only=lambda d: True):
        for d in range(2):
            @pl.when(jnp.logical_and(self.line.sends(d, hop), only(d)))
            def _():
                self.copy(d, c, hop).start()

    def arrive(self, c):
        for hop in range(LINE - 1):
            for d in range(2):
                self.settle(d, c, hop)

    def settle(self, d, c, hop):
        passed_on = self.line.sends(d, hop + 1) if hop + 1 < LINE - 1 else False

        @pl.when(jnp.logical_and(self.line.receives(d, hop), jnp.logical_not(passed_on)))
        def _():
            self.arrival(d, c, hop).wait_recv()

    def relay(self, c, hop, only=lambda d: True, wait=True):
        for d in range(2):
            @pl.when(jnp.logical_and(self.line.sends(d, hop), only(d)))
            def _():
                if wait:
                    self.arrival(d, c, hop - 1).wait_recv()
                self.copy(d, c, hop).start()

    def finish(self, chunks):
        for c in range(chunks):
            for hop in range(LINE - 1):
                for d in range(2):
                    @pl.when(self.line.sends(d, hop))
                    def _():
                        self.copy(d, c, hop).wait_send()


def meet(line, peers):
    barrier = pltpu.get_barrier_semaphore()
    for d in range(2):
        @pl.when(line.exists(d))
        def _():
            pl.semaphore_signal(barrier, inc=1, device_id=line.target(d), device_id_type=MESH)
    for p in peers:
        pl.semaphore_signal(barrier, inc=1, device_id=shift(p), device_id_type=MESH)
    pl.semaphore_wait(barrier, jnp.where(jnp.logical_or(line.z == 0, line.z == LINE - 1), 1, 2) + len(peers))


def normalize(src, dst, gain, bias, start, count):
    block = min(count, LN_ROWS)

    def some(i, _):
        at = pl.ds(pl.multiple_of(start + i * block, RB), block)
        u = src[at, :].astype(f32)
        u = u - jnp.mean(u, axis=-1, keepdims=True)
        var = jnp.mean(u * u, axis=-1, keepdims=True)
        dst[at, :] = (u * lax.rsqrt(var + 1e-6) * gain[...] + bias[...]).astype(bf16)
        return 0

    lax.fori_loop(0, count // block, some, 0)


class Phase:
    def __init__(self, count, copies, compute, after=None, middle=None, before=None):
        self.count, self.copies, self.compute, self.after, self.middle, self.before = count, copies, compute, after, middle, before

    def start(self, n, slot):
        for when, copy in self.copies(n, slot):
            when(copy.start) if when else copy.start()

    def wait(self, n, slot):
        for when, copy in self.copies(n, slot):
            when(copy.wait) if when else copy.wait()


def run_phases(phases, prepare):
    flat = [(p, n) for p in phases for n in range(p.count)]
    ahead = SLOTS - 1
    for i in range(ahead):
        flat[i][0].start(flat[i][1], i)
    prepare()
    base = 0
    for p in phases:
        later = flat[base + p.count : base + p.count + ahead]

        def step(n, _):
            slot = lax.rem(base + n, SLOTS)
            if p.count > ahead:
                @pl.when(n + ahead < p.count)
                def _():
                    p.start(n + ahead, lax.rem(base + n + ahead, SLOTS))
            for j, (q, m) in enumerate(later):
                when = p.count + j - ahead
                if when >= 0:
                    @pl.when(n == when)
                    def _():
                        q.start(m, (base + p.count + j) % SLOTS)
            p.wait(n, slot)
            p.compute(n, slot)
            if p.middle:
                pl.when(n == min(p.count // 2 + 1, p.count - 1))(p.middle)
            return 0

        if p.before:
            p.before()
        if p.count == 1:
            step(0, 0)
        else:
            lax.fori_loop(0, p.count, step, 0)
        if p.after:
            p.after()
        base += p.count


class PlaneGather:
    def __init__(self, line, own, wg, ws, wr, ps, pr, fs, fr):
        width = wg.shape[2]
        cols = width // 8
        self.line, self.wg, self.ps, self.pr, self.fs, self.fr = line, wg, ps, pr, fs, fr
        self.cols = lambda p: pl.ds(pl.multiple_of(p * cols, 128), cols)
        me = shift((0, 0, 0))
        self.place = place_of(me)
        self.core = lax.axis_index("sp") % 2
        self.along = Gather(line, lambda c: own.at[:, self.cols(self.place)], lambda c, o: wg.at[o, :, self.cols(self.place)], ws, wr)
        across, beside = shift(X), shift(Y)
        first_is_x = self.core == 0
        self.diagonal_device = {k: jnp.where(first_is_x, beside[k], across[k]) for k in across}
        self.diagonal_given = jnp.where(first_is_x, place_of(across), place_of(beside))
        self.sources = (place_of(shift(CORE)), place_of(beside), place_of(across), place_of(shift((1, 1, 0))))

    def each(self, hop, action, only=lambda d: True):
        for d in range(2):
            @pl.when(jnp.logical_and(self.line.receives(d, hop), only(d)))
            def _():
                o = jnp.clip(self.line.origin(d, hop + 1), 0, LINE - 1)
                action(d, lambda p: self.wg.at[o, :, self.cols(p)])

    def direct(self, d, hop, k, ref):
        return remote(ref, ref, self.ps.at[d, hop, k], self.pr.at[d, hop, k], shift((CORE, Y, X)[k]))

    def diagonal(self, d, hop, ref):
        return remote(ref, ref, self.ps.at[d, hop, 3], self.pr.at[d, hop, 3], self.diagonal_device)

    def pass_on(self, d, hop, k, ref):
        return remote(ref, ref, self.fs.at[d, hop, k - 1], self.fr.at[d, hop, k - 1], shift(CORE))

    def spread(self, hop, only=lambda d: True, wait="unless relayed"):
        def action(d, slab):
            if wait == "always":
                self.along.arrival(d, 0, hop).wait_recv()
            elif wait == "unless relayed":
                self.along.settle(d, 0, hop)
            for k in range(3):
                self.direct(d, hop, k, slab(self.place)).start()

        self.each(hop, action, only)

    def forward(self, hop, only=lambda d: True):
        def action(d, slab):
            for k in (1, 2):
                self.direct(d, hop, k, slab(self.sources[k])).wait_recv()
                self.pass_on(d, hop, k, slab(self.sources[k])).start()
            self.diagonal(d, hop, slab(self.diagonal_given)).start()

        self.each(hop, action, only)

    def forward_diagonal(self, hop, only=lambda d: True):
        def action(d, slab):
            self.diagonal(d, hop, slab(self.sources[3])).wait_recv()
            self.pass_on(d, hop, 3, slab(self.sources[3])).start()

        self.each(hop, action, only)

    def arrive(self, hops):
        for hop in hops:
            def action(d, slab):
                self.direct(d, hop, 0, slab(self.sources[0])).wait_recv()
                for k in (1, 2, 3):
                    p = self.sources[k]
                    self.pass_on(d, hop, k, slab(p + 1 - 2 * (p % 2))).wait_recv()

            self.each(hop, action)

    def finish(self, hops):
        for hop in hops:
            def action(d, slab):
                for k in range(3):
                    self.direct(d, hop, k, slab(self.place)).wait_send()
                self.diagonal(d, hop, slab(self.diagonal_given)).wait_send()
                for k in (1, 2, 3):
                    self.pass_on(d, hop, k, slab(self.sources[k])).wait_send()

            self.each(hop, action)


def block_kernel(b, step, *refs):
    names = ["x", "gains", "biases", "wq", "wo", "wu", "wd"] + ([] if b == 0 else ["wg_in"])
    names += ["turned", "r", "og", "o", "part"] + (["wg0", "wg1"] if b == 0 else ["wg1"])
    scratch_names = ["rv", "nv", "qkv", "ov", "gv", "mine", "acc", "wbuf", "far_got", "got", "add", "pst"]
    names += scratch_names
    names += ["xs", "xr", "os", "or_", "rs", "rr", "vs", "vr", "ls", "ts", "ds", "hs", "hr", "ws", "wr", "ps", "pr", "fs", "fr"]
    v = dict(zip(names, refs, strict=True))
    x, r, o, og, part, turned = (v[k] for k in ("x", "r", "o", "og", "part", "turned"))
    wq, wo, wu, wd = (v[k] for k in ("wq", "wo", "wu", "wd"))
    rv, nv, qkv, ov, gv, mine, acc, wbuf, far_got, got, add, pst = (v[k] for k in scratch_names)
    rs, rr, vs, vr, ls, ts, ds = (v[k] for k in ("rs", "rr", "vs", "vr", "ls", "ts", "ds"))
    wg = v[f"wg{b}"]
    chunks, rows, width = x.shape
    tokens = rows * LINE
    hk, hidden = wo.shape[1], wu.shape[2]
    heads = hk // 128
    line = Line()
    z = line.z
    xg = Gather(line, lambda c: x.at[c], lambda c, s: r.at[c, s], v["xs"], v["xr"])
    og_ = Gather(line, lambda c: o.at[c], lambda c, s: og.at[c, s], v["os"], v["or_"])
    w0, w1 = (PlaneGather(line, wo.at[i], v[f"wg{i}"], *(v[k].at[i] for k in ("ws", "wr", "ps", "pr", "fs", "fr"))) if i >= b else None for i in range(2))

    def rows_of(o):
        return pl.ds(pl.multiple_of(o * rows, rows), rows)

    def columns(n):
        return pl.ds(pl.multiple_of(n * NB, 128), NB)

    def r_copies(c, own=True):
        return [pltpu.make_async_copy(x.at[c] if own else r.at[c, s], rv.at[rows_of(s), :], ls.at[s]) for s in range(LINE)]

    def load_r(c):
        for s, (a, other) in enumerate(zip(r_copies(c), r_copies(c, False))):
            pl.when(z == s)(a.start)
            pl.when(z != s)(other.start)

    per_tile = NB // 128

    def qkv_phase(c, first, count, wide, middle=None):
        def copies(n, slot):
            return [(None, pltpu.make_async_copy(wq.at[b, (first + n) * per_tile + i], wbuf.at[slot, :, pl.ds(i * 128, 128)], ts.at[slot, i])) for i in range(wide)]

        def compute(n, slot):
            at = pl.ds(pl.multiple_of((first + n) * NB, 128), wide * 128)
            qkv[:, at] = jnp.dot(nv[...], wbuf[slot, :, : wide * 128], preferred_element_type=f32).astype(bf16)

        return Phase(count, copies, compute, None, middle)

    def queries(c, middle=None):
        full, rest = divmod(3 * heads, per_tile)
        phases = [qkv_phase(c, 0, full, per_tile, middle)] + ([qkv_phase(c, full, 1, rest)] if rest else [])

        def piece(o, sem, source):
            return pltpu.make_async_copy(source, rv.at[rows_of(o), :], sem)

        def prepare():
            own = piece(z, ls.at[0], x.at[c])
            own.start()
            before = [(None, own, z)]
            for hop in range(LINE):
                now = []
                if hop < LINE - 1:
                    for d in range(2):
                        origin = jnp.clip(line.origin(d, hop + 1), 0, LINE - 1)
                        now.append((line.receives(d, hop), piece(origin, ls.at[1 + d * (LINE - 1) + hop], r.at[c, origin]), origin))
                        xg.settle(d, c, hop)
                        pl.when(now[-1][0])(now[-1][1].start)
                for there, copy, origin in before:
                    def finish():
                        copy.wait()
                        normalize(rv, nv, v["gains"].at[b, pl.ds(0, 1)], v["biases"].at[b, pl.ds(0, 1)], origin * rows, rows)

                    finish() if there is None else pl.when(there)(finish)
                before = now

        run_phases(phases, prepare)

    def attend(c):
        if step:
            key = lambda t: t // rows * step + t % step
            mask = key(lax.broadcasted_iota(jnp.int32, (tokens, tokens), 0)) == key(lax.broadcasted_iota(jnp.int32, (tokens, tokens), 1))

        def head(h, _):
            at = lambda i: pl.ds(pl.multiple_of((i * heads + h) * 128, 128), 128)
            s = lax.dot_general(qkv[:, at(0)], qkv[:, at(1)], (((1,), (1,)), ((), ())), preferred_element_type=f32) * 128**-0.5
            if step:
                s = jnp.where(mask, s, -1e30)
            e = jnp.exp(s - jnp.max(s, axis=-1, keepdims=True))
            p = (e * (1.0 / jnp.sum(e, axis=-1, keepdims=True))).astype(bf16)
            ov[:, pl.ds(pl.multiple_of(h * 128, 128), 128)] = jnp.dot(p, qkv[:, at(2)], preferred_element_type=f32).astype(bf16)
            return 0

        lax.fori_loop(0, heads, head, 0)
        out = pltpu.make_async_copy(ov, o.at[c], ls.at[2 * LINE])
        out.start()
        out.wait()

    def block_of(i):
        origins = [zz + (hop + 1 if d else -hop - 1) for zz, (d, hop) in enumerate(ARRIVALS[i - 1])]
        return functools.reduce(lambda rest, zz: jnp.where(z == zz, origins[zz], rest), range(LINE), 0)

    def fetch_o(c, i):
        source = o.at[c] if i == 0 else og.at[c, block_of(i)]
        return pltpu.make_async_copy(source, nv.at[:, pl.ds(i * hk, hk)], ls.at[LINE + i])

    def arrive_o(c, i):
        for zz, (d, hop) in enumerate(ARRIVALS[i - 1]):
            pl.when(z == zz)(functools.partial(og_.settle, d, c, hop))
        fetch_o(c, i).start()

    def out_phase(c, i, after):
        wide = 2 if width % (2 * NB) == 0 else 1

        def copies(n, slot):
            source = wo.at[b] if i == 0 else wg.at[block_of(i)]
            return [(None, pltpu.make_async_copy(source.at[:, columns(wide * n + j)], wbuf.at[slot, pl.ds(j * hk, hk), :], ts.at[slot, j])) for j in range(wide)]

        def compute(n, slot):
            for j in range(wide):
                at = columns(wide * n + j)
                a = jnp.dot(nv[:, i * hk : (i + 1) * hk], wbuf[slot, j * hk : (j + 1) * hk, :], preferred_element_type=f32)
                if i > 0:
                    a = acc[:, at] + a
                if i < LINE - 1:
                    acc[:, at] = a
                else:
                    rv[:, at] = (rv[:, at].astype(f32) + a.astype(bf16).astype(f32)).astype(bf16)

        def before():
            fetch_o(c, i).wait()
            if i == LINE - 1:
                for copy in r_copies(c):
                    copy.wait()

        middle = functools.partial(arrive_o, c, i + 1) if i < LINE - 1 else None
        return Phase(width // (wide * NB), copies, compute, after, middle, before)

    def up_phase(after):
        cols = lambda n: pl.ds(pl.multiple_of(jnp.minimum(n * NB, hidden - NB), 128), NB)

        def copies(n, slot):
            return [(None, pltpu.make_async_copy(wu.at[b, :, cols(n)], wbuf.at[slot], ts.at[slot, 0]))]

        def compute(n, slot):
            u = jnp.dot(nv[...], wbuf[slot], preferred_element_type=f32).astype(bf16).astype(f32)
            gv[:, cols(n)] = jax.nn.gelu(u, approximate=True).astype(bf16)

        return Phase(pl.cdiv(hidden, NB), copies, compute, after)

    def down_phase(c, middle):
        count = width // NB

        def store(n, slot):
            return pltpu.make_async_copy(pst.at[slot], part.at[c, :, columns(n)], ds.at[slot])

        def copies(n, slot):
            return [(None, pltpu.make_async_copy(wd.at[b, :, columns(n)], wbuf.at[slot, pl.ds(0, hidden), :], ts.at[slot, 0]))]

        def compute(n, slot):
            s = lax.rem(n, 2)

            @pl.when(n >= 2)
            def _():
                store(n - 2, s).wait()

            pst[s] = jnp.dot(gv[...], wbuf[slot, :hidden, :], preferred_element_type=f32)
            store(n, s).start()

        def after():
            for n in range(max(count - 2, 0), count):
                store(n, n % 2).wait()

        return Phase(count, copies, compute, after, middle)

    def feed(c, mid_out=None, after_out=None, after_up=None, mid_down=None):
        def prepare():
            load_r(c)
            fetch_o(c, 0).start()

        def out_done():
            normalize(rv, nv, v["gains"].at[b, pl.ds(1, 1)], v["biases"].at[b, pl.ds(1, 1)], 0, tokens)
            mine[c] = rv[rows_of(z), :]
            if after_out:
                after_out()

        phases = [out_phase(c, i, after) for i, after in enumerate((None, mid_out, None, out_done))] + [up_phase(after_up)]
        run_phases(phases + [down_phase(c, mid_down)], prepare)

    def term(c, t):
        return part.at[c, rows_of(t), :]

    def slot_of(d, c, far):
        return far_got.at[c] if far == LINE - 1 else got.at[d, c, LINE - 2 - far]

    def hop_copy(d, c, far, src):
        return remote(src, slot_of(d, c, far), rs.at[d, c, LINE - 1 - far], rr.at[d, c, LINE - 1 - far], line.target(d))

    def first(d):
        return z == 0 if d == 0 else z == LINE - 1

    def far_target(d, far):
        return z + far if d == 0 else z - far

    half = width // 2
    early = width // NB // 2 + 1 < width // NB

    def early_copy(d):
        cols = pl.ds(0, half)
        src = part.at[0, rows_of(LINE - 1 if d == 0 else 0), cols]
        return remote(src, far_got.at[0, :, cols], v["hs"].at[d], v["hr"].at[d], line.target(d))

    def rest_copy(d):
        cols = pl.ds(half, half)
        src = part.at[0, rows_of(LINE - 1 if d == 0 else 0), cols]
        return remote(src, far_got.at[0, :, cols], rs.at[d, 0, 0], rr.at[d, 0, 0], line.target(d))

    def split(c, far):
        return early and c == 0 and far == LINE - 1

    def reduce_early():
        for d in range(2):
            pl.when(first(d))(lambda: early_copy(d).start())

    def reduce_start(c, fars):
        for far in fars:
            for d in range(2):
                @pl.when(first(d))
                def _():
                    copy = rest_copy(d) if split(c, far) else hop_copy(d, c, far, term(c, far if d == 0 else LINE - 1 - far))
                    copy.start()

    def middle(d, far):
        t = far_target(d, far - 1)
        return jnp.logical_and(jnp.logical_not(first(d)), jnp.logical_and(t >= 0, t < LINE))

    def reduce_relay(c, far):
        for d in range(2):
            @pl.when(middle(d, far))
            def _():
                t = jnp.clip(far_target(d, far - 1), 0, LINE - 1)
                fetch = pltpu.make_async_copy(term(c, t), add, ls.at[2 * LINE])
                fetch.start()
                slot = slot_of(d, c, far)
                if split(c, far):
                    early_copy(d).wait_recv()
                    rest_copy(d).wait_recv()
                else:
                    hop_copy(d, c, far, slot).wait_recv()
                fetch.wait()

                def some(i, _):
                    at = pl.ds(pl.multiple_of(i * RB, RB), RB)
                    slot[at, :] = slot[at, :] + add[at, :]
                    return 0

                lax.fori_loop(0, rows // RB, some, 0)
                hop_copy(d, c, far - 1, slot).start()

    part_rows = rows // 4
    sp = lax.axis_index("sp")

    def turn(c, k):
        device = shift((CORE, Y, Y_CORE)[k])
        there = mine.at[c, pl.ds(pl.multiple_of(device["sp"] * part_rows, part_rows), part_rows), :]
        return remote(there, turned.at[sp * 4 + c], vs.at[c, k], vr.at[c, k], device)

    def turn_own(c):
        return pltpu.make_async_copy(mine.at[c, pl.ds(pl.multiple_of(sp * part_rows, part_rows), part_rows), :], turned.at[sp * 4 + c], ds.at[2 + c])

    def turn_arrive(c, k):
        device = shift((CORE, Y, Y_CORE)[k])
        here = turned.at[device["sp"] * 4 + c]
        remote(here, here, vs.at[c, k], vr.at[c, k], device).wait_recv()

    def reduce_finish(c):
        fetch = pltpu.make_async_copy(term(c, z), add, ls.at[2 * LINE])
        fetch.start()
        for d in range(2):
            @pl.when(jnp.logical_not(first(d)))
            def _():
                hop_copy(d, c, 1, slot_of(d, c, 1)).wait_recv()
        fetch.wait()

        def some(i, _):
            at = pl.ds(pl.multiple_of(i * RB, RB), RB)
            for d in range(2):
                @pl.when(jnp.logical_not(first(d)))
                def _():
                    add[at, :] = add[at, :] + got[d, c, LINE - 3, at, :]
            m = add[at, :].astype(bf16)
            mine[c, at, :] = (mine[c, at, :].astype(f32) + m.astype(f32)).astype(bf16)
            return 0

        lax.fori_loop(0, rows // RB, some, 0)
        turn_own(c).start()
        for k in range(3):
            turn(c, k).start()

    def reduce_sent(c):
        for far in range(LINE - 1, 0, -1):
            for d in range(2):
                @pl.when(first(d))
                def _():
                    if split(c, far):
                        early_copy(d).wait_send()
                        rest_copy(d).wait_send()
                    else:
                        hop_copy(d, c, far, term(c, 0)).wait_send()
                if far > 1:
                    @pl.when(middle(d, far))
                    def _():
                        hop_copy(d, c, far - 1, slot_of(d, c, far)).wait_send()

    def settled(c):
        reduce_sent(c)
        turn_own(c).wait()
        for k in range(3):
            turn(c, k).wait_send()
            turn_arrive(c, k)

    outward = lambda d: z == (LINE - 2 if d == 0 else 1)
    inward = lambda d: jnp.logical_not(outward(d))
    inner = lambda d: jnp.logical_and(z > 0, z < LINE - 1)
    outer = lambda d: jnp.logical_not(inner(d))
    both = lambda p, q: (lambda d: jnp.logical_and(p(d), q(d)))

    def later(function):
        return lambda *args, **hooks: functools.partial(function, *args, **hooks)

    def hook(*actions):
        def run():
            for action in actions:
                action()

        return run

    c0, c1, c2, c3 = h0, h1, h2, h3 = range(LINE)
    outwards = (h3, h2, h1)
    XS, XR, OS, OR = later(xg.start), later(xg.relay), later(og_.start), later(og_.relay)
    Q, A, B = later(queries), later(attend), later(feed)
    RS, RR, F = later(reduce_start), later(reduce_relay), later(reduce_finish)
    early_half = reduce_early if early else hook()
    rest = lambda d: jnp.logical_not(first(d))
    ahead = [XS(c, h0, first) for c in (c1, c2, c3)]
    VS, VR = later(w1.along.start), later(w1.along.relay)
    VP, VF, VD = later(w1.spread), later(w1.forward), later(w1.forward_diagonal)

    if b == 0:
        US, UR, UP, UF, UD = (later(f) for f in (w0.along.start, w0.along.relay, w0.spread, w0.forward, w0.forward_diagonal))
        lead = [US(c0, h0), UR(c0, h1), UP(h0), UR(c0, h2), XS(c0, h0), *ahead, VS(c0, h0, first), XR(c0, h1), VS(c0, h0, both(inner, inward))]
        lead += [UP(h1), UF(h0), UP(h2), XR(c0, h2), XS(c1, h0, rest), XR(c1, h1)]
        after_a0, after_q1, after_a1 = [UD(h0), UF(h1), UF(h2)], [UD(h1)], [UD(h2), later(w0.arrive)(range(h3))]
        after_b0, after_b1, after_rr13 = [VP(h0, inner, "always")], [VF(h0, inner)], [VD(h0, inner)]
        in_b2, after_b2 = [VS(c0, h0, both(inner, outward)), VR(c0, h1, outward, False)], [VR(c0, h1, inward, False)]
        tail0 = [VP(h1, inner, "always"), VP(h0, outer)]
        tail1 = [VR(c0, h2, wait=False), VF(h0, outer), VP(h1, outer)]
        tail2 = [VF(h1, inner)]
        tail3 = [VD(h0, outer), VD(h1, inner), VF(h1, outer)]
        last = [VD(h1, outer), later(w1.arrive)(range(h2))] + [later(w1.along.settle)(d, c0, h2) for d in range(h2)]
        last += [later(w1.along.finish)(h1), later(w1.finish)(range(h2))]
        done = [later(w0.along.finish)(h1), later(w0.finish)(range(h3))]
    else:
        lead = [VP(h2, wait="never"), XS(c0, h0), *ahead, XR(c0, h1), XR(c0, h2), XS(c1, h0, rest), XR(c1, h1)]
        after_a0, after_q1, after_a1, last, done = [VF(h2)], [VD(h2)], [later(w1.arrive)((h2,))], [], [later(w1.finish)((h2,))]
        after_b0 = after_b1 = after_rr13 = in_b2 = after_b2 = tail0 = tail1 = tail2 = tail3 = []
    schedule = lead + [Q(c0, middle=XR(c1, h2)), A(c0), OS(c0, h0)] + after_a0 + [OR(c0, h1), Q(c1, middle=OR(c0, h2)), XS(c2, h0, rest)] + after_q1
    schedule += [A(c1), OS(c1, h0, first)] + after_a1
    schedule += [B(c0, mid_out=XR(c2, h1), after_out=XR(c2, h2), after_up=hook(OS(c1, h0, rest), XS(c3, h0, rest)), mid_down=early_half), RS(c0, outwards), OR(c1, h1)]
    schedule += after_b0 + [Q(c2, middle=hook(OR(c1, h2), XR(c3, h1))), A(c2), OS(c2, h0, first)]
    schedule += [B(c1, mid_out=RR(c0, h3), after_out=XR(c3, h2), after_up=hook(OS(c2, h0, rest), RR(c0, h2))), RS(c1, outwards[:h2])] + after_b1
    schedule += [Q(c3, middle=hook(OR(c2, h1), F(c0))), OR(c2, h2), A(c3), OS(c3, h0), RS(c1, outwards[h2:]), RR(c1, h3)] + after_rr13
    schedule += [B(c2, mid_out=OR(c3, h1), after_out=OR(c3, h2), after_up=hook(RR(c1, h2), *in_b2)), RS(c2, outwards)] + after_b2
    schedule += [B(c3, mid_out=RR(c2, h3), after_up=RR(c2, h2)), RS(c3, outwards), F(c1)] + tail0 + tail1 + [RR(c3, h3), F(c2)] + tail2
    done += [later(xg.finish)(chunks), later(og_.finish)(chunks)] + [later(settled)(c) for c in range(c3)]
    schedule += tail3 + [RR(c3, h2)] + done + [F(c3)] + last
    meet(line, (CORE, Y, X, Y_CORE))
    for action in schedule:
        action()
    settled(c3)


ANY = pl.BlockSpec(memory_space=pl.ANY)
VMEM = pl.BlockSpec(memory_space=pltpu.VMEM)
DMA = pltpu.SemaphoreType.DMA


def call_block(b, step, x, gains, biases, wq, wo, wu, wd, wg):
    chunks, rows, width = x.shape
    hk, tokens, hidden = wo.shape[1], rows * LINE, wu.shape[2]
    hops = LINE - 1
    shape = jax.ShapeDtypeStruct
    outs = [shape((4 * chunks, rows // 4, width), bf16), shape((chunks, LINE, rows, width), bf16), shape((chunks, LINE, tokens, hk), bf16)]
    outs += [shape((chunks, tokens, hk), bf16), shape((chunks, tokens, width), f32)]
    line_sems = DMA((2, chunks, hops))
    scratch = [
        pltpu.VMEM((tokens, width), bf16), pltpu.VMEM((tokens, width), bf16), pltpu.VMEM((tokens, 3 * hk), bf16), pltpu.VMEM((tokens, hk), bf16),
        pltpu.VMEM((tokens, hidden), bf16), pltpu.VMEM((chunks, rows, width), bf16), pltpu.VMEM((tokens, width), f32), pltpu.VMEM((SLOTS, width, NB), bf16),
        pltpu.VMEM((chunks, rows, width), f32), pltpu.VMEM((2, chunks, 2, rows, width), f32), pltpu.VMEM((rows, width), f32), pltpu.VMEM((2, tokens, NB), f32),
        line_sems, line_sems, line_sems, line_sems, line_sems, line_sems, DMA((chunks, 3)), DMA((chunks, 3)), DMA((3 * LINE,)), DMA((SLOTS, LINE)), DMA((2 + chunks,)), DMA((2,)), DMA((2,)),
    ]
    outs += [shape((LINE, hk, width), bf16)] * (2 - b)
    scratch += [DMA((2, 2, 1, hops)), DMA((2, 2, 1, hops)), DMA((2, 2, hops, 4)), DMA((2, 2, hops, 4)), DMA((2, 2, hops, 3)), DMA((2, 2, hops, 3))]
    args = [x, gains, biases, wq, wo, wu, wd] + ([] if b == 0 else [wg])
    results = pl.pallas_call(
        functools.partial(block_kernel, b, step),
        out_shape=tuple(outs),
        in_specs=[ANY, VMEM, VMEM] + [ANY] * (len(args) - 3),
        out_specs=tuple(ANY for _ in outs),
        scratch_shapes=scratch,
        input_output_aliases={} if b == 0 else {len(args) - 1: len(outs) - 1},
        compiler_params=pltpu.CompilerParams(collective_id=b, has_side_effects=True, vmem_limit_bytes=VMEM_LIMIT),
        name=f"block_{b}",
    )(*args)
    return results[0], results[-1]


def reorder(a, sizes, order):
    n = a.shape[0] * a.shape[1]
    source = jnp.arange(n).reshape(sizes).transpose(order).reshape(n, 1)
    one_hot = (source == jnp.arange(n)[None]).astype(a.dtype)
    return jnp.dot(one_hot, a.reshape(n, -1), preferred_element_type=f32).astype(a.dtype)


def solution(mesh):
    act_spec = P("data", "sp", "tp", None)
    weight_specs = (P(), P(), P(None, None, None, "tp", None), P(None, "tp", None, None), P(None, None, "tp"), P(None, "tp", None))

    def device_program(x, ln_gain, ln_bias, w_qkv, w_out, w_up, w_down):
        _, frames, rows, width = x.shape
        wq = w_qkv.transpose(0, 2, 3, 1, 4).reshape(2, -1, width, 128)
        wo = w_out.reshape(2, -1, width)
        per = rows // 4
        step = per // 4

        def block(b, r, wg):
            return call_block(b, step if b else 0, r, ln_gain, ln_bias, wq, wo, w_up, w_down, wg)

        spatial, wg = block(0, x[0], None)
        turned = reorder(spatial, (4 * frames, 4, step), (1, 0, 2)).reshape(4, -1, width)
        temporal, _ = block(1, turned, wg)
        return reorder(temporal, (4, 4, frames, step), (2, 0, 1, 3)).reshape(1, frames, rows, width)

    return jax.shard_map(device_program, mesh=mesh, in_specs=(act_spec,) + weight_specs, out_specs=act_spec, check_vma=False)
```
